256 devices in a mesh: track: 4 (over y), tm: 64 (over z, x, core).
Axes of the slice: x: 4, y: 4, z: 8, core: 2. Of those that a mesh axis runs over, the one named last changes fastest.
Arguments:
- observations: float32 [8192, 16, 128], P('tm', 'track'), may hold values from -18 to 18
- dynamics: bfloat16 [256, 128, 128], P('track'), may hold values from -1 to 1
- smoother_gain: bfloat16 [256, 128, 128], P('track'), may hold values from -1 to 1
- gains: bfloat16 [256, 128], P('track'), may hold values from 0 to 1
- regime: int32 [2048], P('tm'), may hold values from 0 to 255
Outputs:
- smoothed: float32 [8192, 16, 128], P('tm', 'track')
The draws below stay inside these ranges and needn't reach their ends.
All inputs are finite; a program needn't handle non-finite values.
Results may differ from the reference program's by a relative error of at most 0.0003.
Values may be sent and summed in bfloat16 or wider, within the bound.
A program may use at most 64 MiB of HBM per device.

```python
import jax
import jax.numpy as jnp
from jax import lax

N = 128
REGIMES = 256
DWELL = 4
STEPS = 8192
TRACKS = 16
BLOCKS = 2048


def orthogonal_set(key):
    normal_mat = jax.random.normal(key, (REGIMES, N, N), jnp.float32)
    q_mat, r_mat = jnp.linalg.qr(normal_mat)
    signs = jnp.sign(jnp.diagonal(r_mat, axis1=1, axis2=2))
    return q_mat * signs[:, None, :]


def draw_dynamics(key, part):
    first_key, second_key = jax.random.split(jax.random.fold_in(key, 11))
    rotation = orthogonal_set(first_key)
    scales = jax.random.uniform(second_key, (REGIMES, N), jnp.float32, 1.0 - 1.6 / STEPS, 1.0)
    return (scales[:, :, None] * rotation).astype(jnp.bfloat16)


def draw_smoother_gain(key, part):
    first_key, second_key = jax.random.split(jax.random.fold_in(key, 23))
    rotation = orthogonal_set(first_key)
    scales = jax.random.uniform(second_key, (REGIMES, N), jnp.float32, 1.0 - 2.4 / STEPS, 1.0)
    return (scales[:, :, None] * rotation).astype(jnp.bfloat16)


def draw_gains(key, part):
    lowest = jnp.log(0.16 / STEPS)
    highest = jnp.log(3.2 / STEPS)
    spread = jax.random.uniform(jax.random.fold_in(key, 37), (REGIMES, N), jnp.float32, 0.0, 1.0)
    values = jnp.exp(lowest + (highest - lowest) * spread)
    return values.astype(jnp.bfloat16)


def plant(values, rng, least, high):
    spot = [jax.random.randint(jax.random.fold_in(rng, axis), (), 0, length) for axis, length in enumerate(values.shape)]
    main_axis = values.shape.index(max(values.shape))
    next_to = spot[:main_axis] + [(spot[main_axis] + 1) % values.shape[main_axis]] + spot[main_axis + 1:]
    return values.at[tuple(spot)].set(least).at[tuple(next_to)].set(high)


def shard_levels(key, extent, cuts, smallest, top_value):
    gain = 1.0
    for axis_at, parts in cuts:
        heights = jax.random.uniform(jax.random.fold_in(jax.random.fold_in(key, 6), axis_at), (parts,), jnp.float32, smallest / len(cuts), top_value / len(cuts))
        gain = gain * jnp.repeat(jnp.exp(heights), extent[axis_at] // parts).reshape((-1,) + (1,) * (len(extent) - 1 - axis_at))
    return gain


def centred(stream_key, shape, deviation, bound, cuts=(), dtype=jnp.bfloat16):
    drawn = jax.random.normal(stream_key, shape, jnp.float32) * deviation
    if len(cuts) > 0:
        drawn = shard_levels(stream_key, shape, cuts, -0.22, 0.18) * drawn
    return jnp.clip(drawn, min=-bound, max=bound).astype(dtype)


def setup_inputs(seed: int = 0) -> dict:
    arg_keys = jax.random.split(jax.random.key(seed), 6)
    return {
        "observations": centred(arg_keys[0], (STEPS, TRACKS, N), 3.0, 18.0, ((0, 64), (1, 4)), jnp.float32),
        "dynamics": draw_dynamics(jax.random.fold_in(arg_keys[5], 71), 0),
        "smoother_gain": draw_smoother_gain(jax.random.fold_in(arg_keys[5], 71), 0),
        "gains": draw_gains(jax.random.fold_in(arg_keys[5], 71), 0),
        "regime": plant(jax.random.randint(arg_keys[4], (BLOCKS,), 0, REGIMES), jax.random.fold_in(arg_keys[4], 1), 0, REGIMES - 1).astype(jnp.int32),
    }


def matmul(left, right):
    return jnp.dot(left, right, precision=lax.Precision.HIGHEST)

def reference(observations, dynamics, smoother_gain, gains, regime):
    step_ids = jnp.repeat(regime, DWELL).astype(jnp.int32)
    next_ids = jnp.concatenate([step_ids[1:], jnp.zeros((1,), jnp.int32)])
    live = (jnp.arange(STEPS) < STEPS - 1).astype(jnp.float32)

    def forward(state, inputs):
        measured, which = inputs
        trans = dynamics[which].astype(jnp.float32)
        gain_vec = gains[which].astype(jnp.float32)
        closed = (1.0 - gain_vec)[:, None] * trans
        state = matmul(state, closed.T) + gain_vec[None, :] * measured
        return (state, state)
    start = jnp.zeros((TRACKS, N), jnp.float32)
    _, filtered = lax.scan(forward, start, (observations, step_ids))

    def backward(after, inputs):
        current, which, keep = inputs
        trans = dynamics[which].astype(jnp.float32)
        gain_mat = smoother_gain[which].astype(jnp.float32) * keep
        cross = matmul(gain_mat, trans)
        value = current - matmul(current, cross.T) + matmul(after, gain_mat.T)
        return (value, value)
    _, smoothed = lax.scan(backward, start, (filtered, next_ids, live), reverse=True)
    return smoothed
```

```python
import functools

import jax
import jax.numpy as jnp
import numpy as np
from jax import lax
from jax.experimental import pallas as pl
from jax.experimental.pallas import tpu as pltpu
from jax.sharding import Mesh
from jax.sharding import PartitionSpec as P

TM = ("tm_0", "tm_1", "tm_2")
F32 = jnp.float32
BF16 = jnp.bfloat16
N = 128
TR = 16
ROWS = N + TR
MAP = 2 * ROWS + N
SEGS = 4
MESH = pl.DeviceIdType.MESH
VMEM = pltpu.MemorySpace.VMEM


def split2(x):
    hi = x.astype(BF16)
    return hi, (x - hi.astype(F32)).astype(BF16)


def split3(x):
    hi = x.astype(BF16)
    rest = x - hi.astype(F32)
    mid = rest.astype(BF16)
    return hi, mid, (rest - mid.astype(F32)).astype(BF16)


def dot_t(left, right):
    return lax.dot_general(left, right, (((1,), (1,)), ((), ())), preferred_element_type=F32)


def times_t(x, w):
    hi, mid, low = split3(x)
    return dot_t(jnp.concatenate([hi, mid], axis=1), jnp.concatenate([w, w], axis=1)) + dot_t(low, w)


def product(x, w):
    xh, xl = split2(x)
    wh, wl = split2(w)
    return jnp.dot(
        jnp.concatenate([xh, xl, xh], axis=1),
        jnp.concatenate([wh, wh, wl], axis=0),
        preferred_element_type=F32,
    )


PHI, V_ROW, W_MAT, W_ROW, PSI = 0, N, ROWS, ROWS + N, 2 * ROWS
AHEAD, BEHIND = (0, ROWS), (ROWS, MAP - ROWS)


def compose_ahead(left, right, out):
    both = product(left[pl.ds(0, ROWS)], right[pl.ds(PHI, N)])
    out[pl.ds(0, N)] = both[:N]
    out[pl.ds(V_ROW, TR)] = both[N:] + right[pl.ds(V_ROW, TR)]


def compose_behind(left, right, out):
    both = product(left[pl.ds(0, ROWS)], right[pl.ds(W_MAT, N)])
    last = both[N:] + right[pl.ds(W_ROW, TR)]
    back = product(jnp.concatenate([both[:N], last, right[pl.ds(PSI, N)]], axis=0), left[pl.ds(PSI, N)])
    out[pl.ds(W_MAT, ROWS)] = back[:ROWS] + left[pl.ds(W_MAT, ROWS)]
    out[pl.ds(PSI, N)] = back[ROWS:]


def middle_x(x, left):
    return product(x, left[pl.ds(PHI, N)]) + left[pl.ds(V_ROW, TR)]


def middle_u(x_mid, u, right):
    mats = jnp.concatenate([right[pl.ds(W_MAT, N)], right[pl.ds(PSI, N)]], axis=0)
    return product(jnp.concatenate([x_mid, u], axis=1), mats) + right[pl.ds(W_ROW, TR)]


def tree_of(leaves, nodes):
    levels, used = [leaves], 0
    while len(levels[-1]) > 1:
        row = [nodes.at[used + i] for i in range(len(levels[-1]) // 2)]
        used += len(row)
        levels.append(row)
    return levels


def fill(levels, compose):
    for below, row in zip(levels, levels[1:]):
        for i, node in enumerate(row):
            compose(below[2 * i], below[2 * i + 1], node)


def descend(x, u, levels, position):
    for level in range(len(levels) - 2, -1, -1):
        row = levels[level]
        bit = lax.rem(lax.div(position, 2**level), 2)
        above = lax.div(position, 2 ** (level + 1))
        best_x, best_u = None, None
        for i in range(len(row) // 2):
            x_mid = middle_x(x, row[2 * i])
            u_mid = middle_u(x_mid, u, row[2 * i + 1])
            best_x = x_mid if best_x is None else jnp.where(above == i, x_mid, best_x)
            best_u = u_mid if best_u is None else jnp.where(above == i, u_mid, best_u)
        x = jnp.where(bit == 1, best_x, x)
        u = jnp.where(bit == 1, u, best_u)
    return x, u


class Wires:
    def __init__(self, send, recv):
        self.send, self.recv, self.used = send, recv, 0
        self.pending = []

    def make(self, src, dst, **peer):
        copy = pltpu.make_async_remote_copy(
            src_ref=src,
            dst_ref=dst,
            send_sem=self.send.at[self.used],
            recv_sem=self.recv.at[self.used],
            device_id=peer,
            device_id_type=MESH,
        )
        self.used += 1
        return copy

    def go(self, src, dst, **peer):
        copy = self.make(src, dst, **peer)
        copy.start()
        self.pending.append(copy)
        return copy

    def close(self):
        for copy in self.pending:
            copy.wait_send()


def compose_psi(left, right, out):
    out[pl.ds(PSI, N)] = product(right[pl.ds(PSI, N)], left[pl.ds(PSI, N)])


def compose_w(left, right, out):
    both = product(left[pl.ds(0, ROWS)], right[pl.ds(W_MAT, N)])
    last = both[N:] + right[pl.ds(W_ROW, TR)]
    back = product(jnp.concatenate([both[:N], last], axis=0), left[pl.ds(PSI, N)])
    out[pl.ds(W_MAT, ROWS)] = back + left[pl.ds(W_MAT, ROWS)]


class Ring:
    def __init__(self, wires, buf, axis, size, first, count):
        self.wires, self.buf, self.axis, self.size = wires, buf, axis, size
        self.me = lax.axis_index(axis)
        half = -(-count // 16) * 8
        self.rows = [pl.ds(first, count)]
        if size > 2:
            self.rows = [
                pl.ds(pl.multiple_of(first, 8), half),
                pl.ds(pl.multiple_of(first + half, 8), count - half),
            ]

    def send(self, who, part, there):
        piece = self.buf.at[who, self.rows[part]]
        return self.wires.go(piece, piece, **{self.axis: there})

    def start(self):
        if self.size == 2:
            self.rest = [self.send(self.me, 0, 1 - self.me)]
        if self.size > 2:
            self.right = lax.rem(self.me + 1, self.size)
            self.left = lax.rem(self.me + self.size - 1, self.size)
            self.first = [self.send(self.me, 0, self.right), self.send(self.me, 1, self.left)]
            self.rest = [self.send(self.me, 1, self.right), self.send(self.me, 0, self.left)]

    def relay(self):
        if self.size > 2:
            self.first[0].wait_recv()
            self.rest.append(self.send(self.left, 0, self.right))
            self.first[1].wait_recv()
            self.rest.append(self.send(self.right, 1, self.left))

    def finish(self):
        if self.size > 1:
            for copy in self.rest:
                copy.wait_recv()


class Merge:
    def __init__(self, wires, cand, relay, arrived, y):
        self.wires, self.cand, self.relay_buf, self.arrived, self.y = wires, cand, relay, arrived, y
        self.right, self.left, self.far = (lax.rem(y + k, 4) for k in (1, 3, 2))
        self.each = cand.shape[0] // 4
        self.half = self.each // 2

    def part(self, owner, side):
        return pl.ds(owner * self.each + side * self.half, self.half)

    def start(self):
        go, cand, half = self.wires.go, self.cand, self.half
        low, high = pl.ds(0, half), pl.ds(half, half)
        self.via = [
            go(cand.at[self.part(self.far, 0)], self.relay_buf.at[0], track=self.right),
            go(cand.at[self.part(self.far, 1)], self.relay_buf.at[1], track=self.left),
        ]
        self.rest = [
            go(cand.at[self.part(self.right, 1)], self.arrived.at[0, high], track=self.right),
            go(cand.at[self.part(self.left, 0)], self.arrived.at[1, low], track=self.left),
        ]

    def relay(self):
        go, half = self.wires.go, self.half
        for side, (there, rows) in enumerate(((self.right, pl.ds(0, half)), (self.left, pl.ds(half, half)))):
            self.via[side].wait_recv()
            self.relay_buf[2 + side] = self.relay_buf[side] + self.cand[self.part(there, side)]
            self.rest.append(go(self.relay_buf.at[2 + side], self.arrived.at[side, rows], track=there))

    def finish(self, out):
        for copy in self.rest:
            copy.wait_recv()
        out[...] = self.cand[pl.ds(self.y * self.each, self.each)] + (self.arrived[0] + self.arrived[1])


def forward_pass(a_own, k_own, o_all, x_all, e_all):
    count = a_own.shape[0]
    dwell = o_all.shape[0] // count
    per = count // SEGS
    eye = (
        lax.broadcasted_iota(jnp.int32, (N, N), 0) == lax.broadcasted_iota(jnp.int32, (N, N), 1)
    ).astype(F32)
    start = jnp.concatenate([eye, jnp.zeros((TR, N), F32)], axis=0)
    blank = jnp.zeros((N, N), F32)

    def some(i, xs):
        new_x = list(xs)
        for step in range(dwell):
            for seg in range(SEGS):
                block = seg * per + i
                t = block * dwell + step
                pred = times_t(new_x[seg], a_own[block])
                obs = jnp.concatenate([blank, o_all[t]], axis=0)
                e = k_own[pl.ds(block, 1)] * (obs - pred)
                e_all[t] = e
                x_all[t] = pred + e
                new_x[seg] = pred + e
        return tuple(new_x)

    return lax.fori_loop(0, per, some, (start,) * SEGS)


def backward_pass(g_own, x_all, e_all, hi_ref, lo_ref, s_all):
    count = g_own.shape[0]
    dwell = x_all.shape[0] // count
    per = count // SEGS
    eye = (
        lax.broadcasted_iota(jnp.int32, (N, N), 0) == lax.broadcasted_iota(jnp.int32, (N, N), 1)
    ).astype(F32)

    def keep(t, row, value):
        hi, low = split2(value)
        hi_ref[t, pl.ds(row, N)] = hi
        lo_ref[t, pl.ds(row, N)] = low

    def some(i, carry):
        new_u, new_p = list(carry[0]), list(carry[1])
        for step in range(dwell):
            for seg in range(SEGS):
                block = seg * per + per - 1 - i
                t = block * dwell + dwell - 1 - step
                s = x_all[t] + new_u[seg]
                keep(t, 0, s[:N])
                keep(t, N, new_p[seg])
                s_all[t] = s[N:]
                back = times_t(jnp.concatenate([new_u[seg] + e_all[t], new_p[seg]], axis=0), g_own[block])
                new_u[seg], new_p[seg] = back[:ROWS], back[ROWS:]
        return tuple(new_u), tuple(new_p)

    return lax.fori_loop(0, per, some, ((jnp.zeros((ROWS, N), F32),) * SEGS, (eye,) * SEGS))


def final_pass(x, u, levels, hi_ref, lo_ref, s_all, out_buf, sent):
    spans = [(x, u)]
    for row in levels[-2::-1]:
        new = []
        for i, (x, u) in enumerate(spans):
            x_mid = middle_x(x, row[2 * i])
            new += [(x, middle_u(x_mid, u, row[2 * i + 1])), (x_mid, u)]
        spans = new
    per = s_all.shape[0] // SEGS
    four = TR // 4
    for seg, (x, u) in enumerate(spans):
        hi, low = split2(jnp.concatenate([x, u], axis=1))
        both = jnp.concatenate([hi, low], axis=0)
        for pair in range(per // 2):
            outs = []
            for t in (seg * per + 2 * pair, seg * per + 2 * pair + 1):
                first = jnp.dot(both, hi_ref[t], preferred_element_type=F32)
                second = jnp.dot(hi, lo_ref[t], preferred_element_type=F32)
                outs.append(s_all[t] + ((first[:TR] + first[TR:]) + second))
            for group in range(4):
                rows = slice(four * group, four * group + four)
                out_buf[group, pl.ds((seg * per + 2 * pair) * four, 2 * four)] = jnp.concatenate(
                    [outs[0][rows], outs[1][rows]], axis=0
                )
        sent(seg * per * four, per * four)


def main_kernel(sizes, *refs):
    (ids, dyn, smooth, gain, obs_in, out_ref, tab_a, tab_g, tab_s, tab_k, ca, cg, ck, local, relay, arrived, k_buf, o_buf, o_way, a_own, g_own, k_own, o_all, x_all, e_all,
     hi_ref, lo_ref, s_all, segs, segnode, ybuf, ynode, cbuf, cnode, xbuf, xnode, zpv, zps, zc, out_buf,
     send, recv) = refs
    ny, nz, nx, nc = sizes
    y, z, x, c = (lax.axis_index(a) for a in ("track",) + TM)
    each = obs_in.shape[0] // 4
    blocks = a_own.shape[0]
    own_rows = pl.ds(pl.multiple_of(y * each, each), each)
    fetch_a = pltpu.make_async_copy(dyn, tab_a, local.at[0])
    fetch_g = pltpu.make_async_copy(smooth, tab_g, local.at[1])
    fetch_o = pltpu.make_async_copy(obs_in.at[own_rows], o_buf.at[y], local.at[2])
    fetch_k = pltpu.make_async_copy(gain, tab_s, local.at[3])
    for copy in (fetch_k, fetch_a, fetch_g, fetch_o):
        copy.start()
    barrier = pltpu.get_barrier_semaphore()
    peers = []
    for axis, me, size in (("track", y, ny), ("tm_0", z, nz), ("tm_1", x, nx), ("tm_2", c, nc)):
        for step in range(1, size):
            peers.append({axis: lax.rem(me + step, size)})
    for peer in peers:
        pl.semaphore_signal(barrier, inc=1, device_id=peer, device_id_type=MESH)
    fetch_k.wait()
    tab_k[...] = tab_s[...].astype(F32)
    owned = tab_a.shape[0]
    zero_mat = jnp.zeros((N, N), BF16)

    def picked(b):
        row = ids[b] - y * owned
        return jnp.logical_and(row >= 0, row < owned), jnp.clip(row, 0, owned - 1)

    def pick_a(b, _):
        here, row = picked(b)
        ca[b] = jnp.where(here, tab_a[row], zero_mat)
        ck[pl.ds(b, 1)] = jnp.where(here, tab_k[pl.ds(row, 1)], 0.0)
        return 0

    def pick_g(b, _):
        here, row = picked(b)
        cg[b] = jnp.where(here, tab_g[row], zero_mat)
        return 0

    fetch_a.wait()
    lax.fori_loop(0, ca.shape[0], pick_a, 0)
    pl.semaphore_wait(barrier, len(peers))
    wires = Wires(send, recv)
    right, left, far = others = [lax.rem(y + k, 4) for k in (1, 3, 2)]

    a_move = Merge(wires, ca, relay.at[0], arrived.at[0], y)
    g_move = Merge(wires, cg, relay.at[1], arrived.at[1], y)
    a_move.start()
    small = []
    half = each // 2

    def obs_rows(owner, first, count):
        return obs_in.at[pl.ds(pl.multiple_of(owner * each + first, 8), count)]

    for there in (right, left):
        small.append(wires.go(obs_rows(there, 0, each), o_buf.at[y], track=there))
    small.append(wires.go(obs_rows(far, 0, half), o_buf.at[y, pl.ds(0, half)], track=far))
    detour = wires.go(obs_rows(far, half, half), o_way.at[0], track=left)
    for there in others:
        small.append(wires.go(ck.at[pl.ds(pl.multiple_of(there * blocks, blocks), blocks)], k_buf.at[y], track=there))
    k_buf[y] = ck[pl.ds(pl.multiple_of(y * blocks, blocks), blocks)]
    fetch_g.wait()
    lax.fori_loop(0, cg.shape[0], pick_g, 0)
    a_move.relay()
    detour.wait_recv()
    small.append(wires.go(o_way.at[0], o_buf.at[right, pl.ds(half, half)], track=left))
    g_move.start()
    a_move.finish(a_own)
    for copy in small:
        copy.wait_recv()
    fetch_o.wait()
    k_own[...] = (k_buf[0] + k_buf[1]) + (k_buf[2] + k_buf[3])
    four = TR // 4

    def in_steps(p, _):
        tiles = [o_buf[s, pl.ds(pl.multiple_of(p * 2 * four, 8), 2 * four)] for s in range(4)]
        o_all[2 * p] = jnp.concatenate([tile[:four] for tile in tiles], axis=0)
        o_all[2 * p + 1] = jnp.concatenate([tile[four:] for tile in tiles], axis=0)
        return 0

    lax.fori_loop(0, each // (2 * four), in_steps, 0)

    xs = forward_pass(a_own, k_own, o_all, x_all, e_all)
    for seg in range(SEGS):
        segs[seg, pl.ds(0, ROWS)] = xs[seg]
    stree = tree_of([segs.at[i] for i in range(SEGS)], segnode)
    ytree = tree_of([ybuf.at[i] for i in range(ny)], ynode)
    ctree = tree_of([cbuf.at[i] for i in range(nc)], cnode)
    xtree = tree_of([xbuf.at[i] for i in range(nx)], xnode)
    share_a, share_b = AHEAD[1] // nc, BEHIND[1] // nc
    own_a, own_b = c * share_a, BEHIND[0] + c * share_b
    y_ahead = Ring(wires, ybuf, "track", ny, *AHEAD)
    y_behind = Ring(wires, ybuf, "track", ny, *BEHIND)
    c_ahead = Ring(wires, cbuf, "tm_2", nc, *AHEAD)
    c_behind = Ring(wires, cbuf, "tm_2", nc, *BEHIND)
    x_ahead = Ring(wires, xbuf, "tm_1", nx, own_a, share_a)
    x_behind = Ring(wires, xbuf, "tm_1", nx, own_b, share_b)
    fill(stree, compose_ahead)
    ybuf[y, pl.ds(0, ROWS)] = stree[-1][0][pl.ds(0, ROWS)]
    g_move.relay()
    y_ahead.start()
    g_move.finish(g_own)
    y_ahead.relay()

    us, ps = backward_pass(g_own, x_all, e_all, hi_ref, lo_ref, s_all)
    for seg in range(SEGS):
        segs[seg, pl.ds(W_MAT, ROWS)] = us[seg]
        segs[seg, pl.ds(PSI, N)] = ps[seg]
    fill(stree, compose_behind)
    ybuf[y, pl.ds(W_MAT, ROWS + N)] = stree[-1][0][pl.ds(W_MAT, ROWS + N)]
    y_behind.start()

    def share_start(own, share):
        rows = pl.ds(pl.multiple_of(own, 8), share)
        parts = [xbuf.at[lax.rem(x + step, nx), rows] for step in range(1, nx)] if nc > 1 else []
        return [wires.go(part, part, tm_2=1 - c) for part in parts]

    def to_slabs(buf, rows, later):
        mine = pl.ds(pl.multiple_of(c * (rows // nc), 8), rows // nc)
        part = buf.at[z, mine]
        moves = []
        for step in range(1, nz):
            there = z + step if later else z - step
            copy = wires.make(part, part, tm_0=jnp.clip(there, 0, nz - 1))
            use = there < nz if later else there >= 0
            moves.append((copy, use))
            pl.when(use)(copy.start)
        return mine, moves

    def from_slabs(buf, mine, moves, later):
        shared = []
        for step, (copy, _) in enumerate(moves, 1):
            source = z - step if later else z + step
            use = source >= 0 if later else source < nz
            pl.when(use)(copy.wait_recv)
            if nc > 1:
                part = buf.at[jnp.clip(source, 0, nz - 1), mine]
                over = wires.make(part, part, tm_2=1 - c)
                pl.when(use)(over.start)
                shared.append((over, use))
        for copy, use in shared:
            pl.when(use)(copy.wait_recv)
        for copy, use in moves + shared:
            pl.when(use)(copy.wait_send)

    y_ahead.finish()
    fill(ytree, compose_ahead)
    cbuf[c, pl.ds(0, ROWS)] = ytree[-1][0][pl.ds(0, ROWS)]
    c_ahead.start()
    c_ahead.finish()
    fill(ctree, compose_ahead)
    xbuf[x, pl.ds(0, ROWS)] = ctree[-1][0][pl.ds(0, ROWS)]
    x_ahead.start()
    y_behind.relay()
    x_ahead.relay()
    y_behind.finish()
    fill(ytree, compose_behind)
    cbuf[c, pl.ds(W_MAT, ROWS + N)] = ytree[-1][0][pl.ds(W_MAT, ROWS + N)]
    c_behind.start()
    x_ahead.finish()
    shared = share_start(own_a, share_a)
    c_behind.finish()
    fill(ctree, compose_behind)
    xbuf[x, pl.ds(W_MAT, ROWS + N)] = ctree[-1][0][pl.ds(W_MAT, ROWS + N)]
    x_behind.start()
    for copy in shared:
        copy.wait_recv()
    fill(xtree, compose_ahead)
    total = xtree[-1][0]
    zpv[z] = total[pl.ds(0, ROWS)]
    z_ahead = to_slabs(zpv, ROWS, True)
    x_behind.relay()
    x_behind.finish()
    for copy in share_start(own_b, share_b):
        copy.wait_recv()
    fill(xtree, compose_psi)
    zps[z] = total[pl.ds(PSI, N)]
    z_behind = to_slabs(zps, N, False)
    fill(xtree, compose_w)
    from_slabs(zpv, *z_ahead, True)

    zero = jnp.zeros((TR, N), F32)
    entering, state = zero, zero
    for i in range(nz - 1):
        got = jnp.minimum(i, z)
        after = zpv[got, pl.ds(V_ROW, TR)]
        if i > 0:
            after = after + product(state, zpv[got, pl.ds(PHI, N)])
        state = after
        entering = jnp.where(z == i + 1, state, entering)
    zc[z] = product(entering, total[pl.ds(W_MAT, N)]) + total[pl.ds(W_ROW, TR)]
    part = zc.at[z]
    group = [wires.go(part, part, tm_0=lax.rem(z + step, nz)) for step in range(1, nz)]
    from_slabs(zps, *z_behind, False)
    for copy in group:
        copy.wait_recv()
    leaving, state = zero, zero
    for i in range(nz - 1, 0, -1):
        after = zc[i]
        if i < nz - 1:
            after = after + product(state, zps[jnp.maximum(i, z)])
        state = after
        leaving = jnp.where(z == i - 1, state, leaving)

    xv, uv = descend(entering, leaving, xtree, x)
    xv, uv = descend(xv, uv, ctree, c)
    xv, uv = descend(xv, uv, ytree, y)

    homes, detours = [], []

    def target(first, count):
        return out_ref.at[pl.ds(pl.multiple_of(y * each + first, 8), count)]

    def sent(first, count):
        rows = pl.ds(first, count)
        if first < half:
            detours.append((wires.go(out_buf.at[far, rows], o_way.at[1, rows], track=left), rows, first, count))
        for there in (right, left) if first < half else others:
            homes.append(wires.go(out_buf.at[there, rows], target(first, count), track=there))

    final_pass(xv, uv, stree, hi_ref, lo_ref, s_all, out_buf, sent)
    out_ref[own_rows] = out_buf[y]
    for copy, rows, first, count in detours:
        copy.wait_recv()
        there = out_ref.at[pl.ds(pl.multiple_of(right * each + first, 8), count)]
        homes.append(wires.go(o_way.at[1, rows], there, track=left))
    for copy in homes:
        copy.wait_recv()
    wires.close()


def main_call(sizes, ids, dyn, smooth, gain, obs):
    ny, nz, nx, nc = sizes
    count, owned = ids.shape[0], dyn.shape[0]
    blocks = count // ny
    each = obs.shape[0] // ny
    steps = each // (TR // ny)
    links = 20 + 30 + 2 * (1 + nx) + 5 * nz + 3 * SEGS
    hbm = pl.BlockSpec(memory_space=pltpu.MemorySpace.HBM)
    vmem = pl.BlockSpec(memory_space=VMEM)
    return pl.pallas_call(
        functools.partial(main_kernel, sizes),
        out_shape=jax.ShapeDtypeStruct(obs.shape, F32),
        in_specs=[pl.BlockSpec(memory_space=pltpu.MemorySpace.SMEM), hbm, hbm, hbm, hbm],
        out_specs=vmem,
        scratch_shapes=[
            pltpu.VMEM((owned, N, N), BF16),
            pltpu.VMEM((owned, N, N), BF16),
            pltpu.VMEM((owned, N), BF16),
            pltpu.VMEM((owned, N), F32),
            pltpu.VMEM((count, N, N), BF16),
            pltpu.VMEM((count, N, N), BF16),
            pltpu.VMEM((count, N), F32),
            pltpu.SemaphoreType.DMA((4,)),
            pltpu.VMEM((2, 4, blocks // 2, N, N), BF16),
            pltpu.VMEM((2, 2, blocks, N, N), BF16),
            pltpu.VMEM((4, blocks, N), F32),
            pltpu.VMEM((4, each, N), F32),
            pltpu.VMEM((2, each // 2, N), F32),
            pltpu.VMEM((blocks, N, N), BF16),
            pltpu.VMEM((blocks, N, N), BF16),
            pltpu.VMEM((blocks, N), F32),
            pltpu.VMEM((steps, TR, N), F32),
            pltpu.VMEM((steps, ROWS, N), F32),
            pltpu.VMEM((steps, ROWS, N), F32),
            pltpu.VMEM((steps, 2 * N, N), BF16),
            pltpu.VMEM((steps, 2 * N, N), BF16),
            pltpu.VMEM((steps, TR, N), F32),
            pltpu.VMEM((SEGS, MAP, N), F32),
            pltpu.VMEM((SEGS - 1, MAP, N), F32),
            pltpu.VMEM((ny, MAP, N), F32),
            pltpu.VMEM((max(ny - 1, 1), MAP, N), F32),
            pltpu.VMEM((nc, MAP, N), F32),
            pltpu.VMEM((max(nc - 1, 1), MAP, N), F32),
            pltpu.VMEM((nx, MAP, N), F32),
            pltpu.VMEM((max(nx - 1, 1), MAP, N), F32),
            pltpu.VMEM((nz, ROWS, N), F32),
            pltpu.VMEM((nz, N, N), F32),
            pltpu.VMEM((nz, TR, N), F32),
            pltpu.VMEM((4, each, N), F32),
            pltpu.SemaphoreType.DMA((links,)),
            pltpu.SemaphoreType.DMA((links,)),
        ],
        compiler_params=pltpu.CompilerParams(
            collective_id=1, has_side_effects=True, vmem_limit_bytes=67043328
        ),
        name="smooth",
    )(ids, dyn, smooth, gain, obs)


def body(sizes, observations, dynamics, smoother_gain, gains, regime):
    out = main_call(sizes, regime, dynamics, smoother_gain, gains, observations.reshape(-1, N))
    return out.reshape(observations.shape)


def build(torus):
    sizes = tuple(torus.shape[a] for a in ("track",) + TM)
    placed = (
        P(TM, "track", None),
        P("track", None, None),
        P("track", None, None),
        P("track", None),
        P(TM),
    )
    return jax.shard_map(
        functools.partial(body, sizes),
        mesh=torus,
        in_specs=placed,
        out_specs=P(TM, "track", None),
        check_vma=False,
    )


def solution(mesh):
    return build(Mesh(mesh.devices.reshape(mesh.shape["track"], 8, 4, 2), ("track",) + TM))
```

```python
import functools

import jax
import jax.numpy as jnp
import numpy as np
from jax import lax
from jax.experimental import pallas as pl
from jax.experimental.pallas import tpu as pltpu
from jax.sharding import Mesh
from jax.sharding import PartitionSpec as P

TM = ("tm_0", "tm_1", "tm_2")
F32 = jnp.float32
BF16 = jnp.bfloat16
N = 128
TR = 16
ROWS = N + TR
MAP = 2 * ROWS + N
SEGS = 4
MESH = pl.DeviceIdType.MESH
VMEM = pltpu.MemorySpace.VMEM


def split2(x):
    hi = x.astype(BF16)
    return hi, (x - hi.astype(F32)).astype(BF16)


def split3(x):
    hi = x.astype(BF16)
    rest = x - hi.astype(F32)
    mid = rest.astype(BF16)
    return hi, mid, (rest - mid.astype(F32)).astype(BF16)


def dot_t(left, right):
    return lax.dot_general(left, right, (((1,), (1,)), ((), ())), preferred_element_type=F32)


def times_t(x, w):
    hi, mid, low = split3(x)
    return dot_t(jnp.concatenate([hi, mid], axis=1), jnp.concatenate([w, w], axis=1)) + dot_t(low, w)


def product(x, w):
    xh, xl = split2(x)
    wh, wl = split2(w)
    return jnp.dot(
        jnp.concatenate([xh, xl, xh], axis=1),
        jnp.concatenate([wh, wh, wl], axis=0),
        preferred_element_type=F32,
    )


PHI, V_ROW, W_MAT, W_ROW, PSI = 0, N, ROWS, ROWS + N, 2 * ROWS
AHEAD, BEHIND = (0, ROWS), (ROWS, MAP - ROWS)


def compose_ahead(left, right, out):
    both = product(left[pl.ds(0, ROWS)], right[pl.ds(PHI, N)])
    out[pl.ds(0, N)] = both[:N]
    out[pl.ds(V_ROW, TR)] = both[N:] + right[pl.ds(V_ROW, TR)]


def compose_behind(left, right, out):
    both = product(left[pl.ds(0, ROWS)], right[pl.ds(W_MAT, N)])
    last = both[N:] + right[pl.ds(W_ROW, TR)]
    back = product(jnp.concatenate([both[:N], last, right[pl.ds(PSI, N)]], axis=0), left[pl.ds(PSI, N)])
    out[pl.ds(W_MAT, ROWS)] = back[:ROWS] + left[pl.ds(W_MAT, ROWS)]
    out[pl.ds(PSI, N)] = back[ROWS:]


def middle_x(x, left):
    return product(x, left[pl.ds(PHI, N)]) + left[pl.ds(V_ROW, TR)]


def middle_u(x_mid, u, right):
    mats = jnp.concatenate([right[pl.ds(W_MAT, N)], right[pl.ds(PSI, N)]], axis=0)
    return product(jnp.concatenate([x_mid, u], axis=1), mats) + right[pl.ds(W_ROW, TR)]


def tree_of(leaves, nodes):
    levels, used = [leaves], 0
    while len(levels[-1]) > 1:
        row = [nodes.at[used + i] for i in range(len(levels[-1]) // 2)]
        used += len(row)
        levels.append(row)
    return levels


def fill(levels, compose):
    for below, row in zip(levels, levels[1:]):
        for i, node in enumerate(row):
            compose(below[2 * i], below[2 * i + 1], node)


def descend(x, u, levels, position):
    for level in range(len(levels) - 2, -1, -1):
        row = levels[level]
        bit = lax.rem(lax.div(position, 2**level), 2)
        above = lax.div(position, 2 ** (level + 1))
        best_x, best_u = None, None
        for i in range(len(row) // 2):
            x_mid = middle_x(x, row[2 * i])
            u_mid = middle_u(x_mid, u, row[2 * i + 1])
            best_x = x_mid if best_x is None else jnp.where(above == i, x_mid, best_x)
            best_u = u_mid if best_u is None else jnp.where(above == i, u_mid, best_u)
        x = jnp.where(bit == 1, best_x, x)
        u = jnp.where(bit == 1, u, best_u)
    return x, u


class Wires:
    def __init__(self, send, recv):
        self.send, self.recv, self.used = send, recv, 0
        self.pending = []

    def make(self, src, dst, **peer):
        copy = pltpu.make_async_remote_copy(
            src_ref=src,
            dst_ref=dst,
            send_sem=self.send.at[self.used],
            recv_sem=self.recv.at[self.used],
            device_id=peer,
            device_id_type=MESH,
        )
        self.used += 1
        return copy

    def go(self, src, dst, **peer):
        copy = self.make(src, dst, **peer)
        copy.start()
        self.pending.append(copy)
        return copy

    def close(self):
        for copy in self.pending:
            copy.wait_send()


def compose_psi(left, right, out):
    out[pl.ds(PSI, N)] = product(right[pl.ds(PSI, N)], left[pl.ds(PSI, N)])


class Ring:
    def __init__(self, wires, buf, axis, size, first, count):
        self.wires, self.buf, self.axis, self.size = wires, buf, axis, size
        self.me = lax.axis_index(axis)
        half = -(-count // 16) * 8
        self.rows = [pl.ds(first, count)]
        if size > 2:
            self.rows = [
                pl.ds(pl.multiple_of(first, 8), half),
                pl.ds(pl.multiple_of(first + half, 8), count - half),
            ]

    def send(self, who, part, there):
        piece = self.buf.at[who, self.rows[part]]
        return self.wires.go(piece, piece, **{self.axis: there})

    def start(self):
        if self.size == 2:
            self.rest = [self.send(self.me, 0, 1 - self.me)]
        if self.size > 2:
            self.right = lax.rem(self.me + 1, self.size)
            self.left = lax.rem(self.me + self.size - 1, self.size)
            self.first = [self.send(self.me, 0, self.right), self.send(self.me, 1, self.left)]
            self.rest = [self.send(self.me, 1, self.right), self.send(self.me, 0, self.left)]

    def relay(self):
        if self.size > 2:
            self.first[0].wait_recv()
            self.rest.append(self.send(self.left, 0, self.right))
            self.first[1].wait_recv()
            self.rest.append(self.send(self.right, 1, self.left))

    def finish(self):
        if self.size > 1:
            for copy in self.rest:
                copy.wait_recv()


class Merge:
    def __init__(self, wires, cand, relay, arrived, y):
        self.wires, self.cand, self.relay_buf, self.arrived, self.y = wires, cand, relay, arrived, y
        self.right, self.left, self.far = (lax.rem(y + k, 4) for k in (1, 3, 2))
        self.each = cand.shape[0] // 4
        self.half = self.each // 2

    def part(self, owner, side):
        return pl.ds(owner * self.each + side * self.half, self.half)

    def start(self):
        go, cand, half = self.wires.go, self.cand, self.half
        low, high = pl.ds(0, half), pl.ds(half, half)
        self.via = [
            go(cand.at[self.part(self.far, 0)], self.relay_buf.at[0], track=self.right),
            go(cand.at[self.part(self.far, 1)], self.relay_buf.at[1], track=self.left),
        ]
        self.rest = [
            go(cand.at[self.part(self.right, 1)], self.arrived.at[0, high], track=self.right),
            go(cand.at[self.part(self.left, 0)], self.arrived.at[1, low], track=self.left),
        ]

    def relay(self):
        go, half = self.wires.go, self.half
        for side, (there, rows) in enumerate(((self.right, pl.ds(0, half)), (self.left, pl.ds(half, half)))):
            self.via[side].wait_recv()
            self.relay_buf[2 + side] = self.relay_buf[side] + self.cand[self.part(there, side)]
            self.rest.append(go(self.relay_buf.at[2 + side], self.arrived.at[side, rows], track=there))

    def finish(self, out):
        for copy in self.rest:
            copy.wait_recv()
        out[...] = self.cand[pl.ds(self.y * self.each, self.each)] + (self.arrived[0] + self.arrived[1])


def forward_pass(a_own, k_own, o_all, x_all, e_all):
    count = a_own.shape[0]
    dwell = o_all.shape[0] // count
    per = count // SEGS
    eye = (
        lax.broadcasted_iota(jnp.int32, (N, N), 0) == lax.broadcasted_iota(jnp.int32, (N, N), 1)
    ).astype(F32)
    start = jnp.concatenate([eye, jnp.zeros((TR, N), F32)], axis=0)
    blank = jnp.zeros((N, N), F32)

    def some(i, xs):
        new_x = list(xs)
        for step in range(dwell):
            for seg in range(SEGS):
                block = seg * per + i
                t = block * dwell + step
                pred = times_t(new_x[seg], a_own[block])
                obs = jnp.concatenate([blank, o_all[t]], axis=0)
                e = k_own[pl.ds(block, 1)] * (obs - pred)
                e_all[t] = e
                x_all[t] = pred + e
                new_x[seg] = pred + e
        return tuple(new_x)

    return lax.fori_loop(0, per, some, (start,) * SEGS)


def backward_pass(g_own, x_all, e_all, hi_ref, lo_ref, s_all):
    count = g_own.shape[0]
    dwell = x_all.shape[0] // count
    per = count // SEGS
    eye = (
        lax.broadcasted_iota(jnp.int32, (N, N), 0) == lax.broadcasted_iota(jnp.int32, (N, N), 1)
    ).astype(F32)

    def keep(t, row, value):
        hi, low = split2(value)
        hi_ref[t, pl.ds(row, N)] = hi
        lo_ref[t, pl.ds(row, N)] = low

    def some(i, carry):
        new_u, new_p = list(carry[0]), list(carry[1])
        for step in range(dwell):
            for seg in range(SEGS):
                block = seg * per + per - 1 - i
                t = block * dwell + dwell - 1 - step
                s = x_all[t] + new_u[seg]
                keep(t, 0, s[:N])
                keep(t, N, new_p[seg])
                s_all[t] = s[N:]
                back = times_t(jnp.concatenate([new_u[seg] + e_all[t], new_p[seg]], axis=0), g_own[block])
                new_u[seg], new_p[seg] = back[:ROWS], back[ROWS:]
        return tuple(new_u), tuple(new_p)

    return lax.fori_loop(0, per, some, ((jnp.zeros((ROWS, N), F32),) * SEGS, (eye,) * SEGS))


def final_pass(x, u, levels, hi_ref, lo_ref, s_all, out_buf, sent):
    spans = [(x, u)]
    for row in levels[-2::-1]:
        new = []
        for i, (x, u) in enumerate(spans):
            x_mid = middle_x(x, row[2 * i])
            new += [(x, middle_u(x_mid, u, row[2 * i + 1])), (x_mid, u)]
        spans = new
    per = s_all.shape[0] // SEGS
    four = TR // 4
    for seg, (x, u) in enumerate(spans):
        hi, low = split2(jnp.concatenate([x, u], axis=1))
        both = jnp.concatenate([hi, low], axis=0)
        for pair in range(per // 2):
            outs = []
            for t in (seg * per + 2 * pair, seg * per + 2 * pair + 1):
                first = jnp.dot(both, hi_ref[t], preferred_element_type=F32)
                second = jnp.dot(hi, lo_ref[t], preferred_element_type=F32)
                outs.append(s_all[t] + ((first[:TR] + first[TR:]) + second))
            for group in range(4):
                rows = slice(four * group, four * group + four)
                out_buf[group, pl.ds((seg * per + 2 * pair) * four, 2 * four)] = jnp.concatenate(
                    [outs[0][rows], outs[1][rows]], axis=0
                )
        sent(seg * per * four, per * four)


def main_kernel(sizes, *refs):
    (ids, dyn, smooth, gain, obs_in, out_ref, tab_a, tab_g, tab_s, tab_k, ca, cg, ck, local, relay, arrived, k_buf, o_buf, o_way, a_own, g_own, k_own, o_all, x_all, e_all,
     hi_ref, lo_ref, s_all, segs, segnode, ybuf, ynode, cbuf, cnode, xbuf, xnode, zpv, zps, zc, out_buf,
     send, recv) = refs
    ny, nz, nx, nc = sizes
    y, z, x, c = (lax.axis_index(a) for a in ("track",) + TM)
    each = obs_in.shape[0] // 4
    blocks = a_own.shape[0]
    own_rows = pl.ds(pl.multiple_of(y * each, each), each)
    fetch_a = pltpu.make_async_copy(dyn, tab_a, local.at[0])
    fetch_g = pltpu.make_async_copy(smooth, tab_g, local.at[1])
    fetch_o = pltpu.make_async_copy(obs_in.at[own_rows], o_buf.at[y], local.at[2])
    fetch_k = pltpu.make_async_copy(gain, tab_s, local.at[3])
    for copy in (fetch_k, fetch_a, fetch_g, fetch_o):
        copy.start()
    barrier = pltpu.get_barrier_semaphore()
    peers = []
    for axis, me, size in (("track", y, ny), ("tm_0", z, nz), ("tm_1", x, nx), ("tm_2", c, nc)):
        for step in range(1, size):
            peers.append({axis: lax.rem(me + step, size)})
    for peer in peers:
        pl.semaphore_signal(barrier, inc=1, device_id=peer, device_id_type=MESH)
    fetch_k.wait()
    tab_k[...] = tab_s[...].astype(F32)
    owned = tab_a.shape[0]
    zero_mat = jnp.zeros((N, N), BF16)

    def picked(b):
        row = ids[b] - y * owned
        return jnp.logical_and(row >= 0, row < owned), jnp.clip(row, 0, owned - 1)

    def pick_a(b, _):
        here, row = picked(b)
        ca[b] = jnp.where(here, tab_a[row], zero_mat)
        ck[pl.ds(b, 1)] = jnp.where(here, tab_k[pl.ds(row, 1)], 0.0)
        return 0

    def pick_g(b, _):
        here, row = picked(b)
        cg[b] = jnp.where(here, tab_g[row], zero_mat)
        return 0

    fetch_a.wait()
    lax.fori_loop(0, ca.shape[0], pick_a, 0)
    pl.semaphore_wait(barrier, len(peers))
    wires = Wires(send, recv)
    right, left, far = others = [lax.rem(y + k, 4) for k in (1, 3, 2)]

    a_move = Merge(wires, ca, relay.at[0], arrived.at[0], y)
    g_move = Merge(wires, cg, relay.at[1], arrived.at[1], y)
    a_move.start()
    small = []
    half = each // 2

    def obs_rows(owner, first, count):
        return obs_in.at[pl.ds(pl.multiple_of(owner * each + first, 8), count)]

    for there in (right, left):
        small.append(wires.go(obs_rows(there, 0, each), o_buf.at[y], track=there))
    small.append(wires.go(obs_rows(far, 0, half), o_buf.at[y, pl.ds(0, half)], track=far))
    detour = wires.go(obs_rows(far, half, half), o_way.at[0], track=left)
    for there in others:
        small.append(wires.go(ck.at[pl.ds(pl.multiple_of(there * blocks, blocks), blocks)], k_buf.at[y], track=there))
    k_buf[y] = ck[pl.ds(pl.multiple_of(y * blocks, blocks), blocks)]
    fetch_g.wait()
    lax.fori_loop(0, cg.shape[0], pick_g, 0)
    a_move.relay()
    detour.wait_recv()
    small.append(wires.go(o_way.at[0], o_buf.at[right, pl.ds(half, half)], track=left))
    g_move.start()
    a_move.finish(a_own)
    for copy in small:
        copy.wait_recv()
    fetch_o.wait()
    k_own[...] = (k_buf[0] + k_buf[1]) + (k_buf[2] + k_buf[3])
    four = TR // 4

    def in_steps(p, _):
        tiles = [o_buf[s, pl.ds(pl.multiple_of(p * 2 * four, 8), 2 * four)] for s in range(4)]
        o_all[2 * p] = jnp.concatenate([tile[:four] for tile in tiles], axis=0)
        o_all[2 * p + 1] = jnp.concatenate([tile[four:] for tile in tiles], axis=0)
        return 0

    lax.fori_loop(0, each // (2 * four), in_steps, 0)

    xs = forward_pass(a_own, k_own, o_all, x_all, e_all)
    for seg in range(SEGS):
        segs[seg, pl.ds(0, ROWS)] = xs[seg]
    stree = tree_of([segs.at[i] for i in range(SEGS)], segnode)
    ytree = tree_of([ybuf.at[i] for i in range(ny)], ynode)
    ctree = tree_of([cbuf.at[i] for i in range(nc)], cnode)
    xtree = tree_of([xbuf.at[i] for i in range(nx)], xnode)
    share_a, share_b = AHEAD[1] // nc, BEHIND[1] // nc
    own_a, own_b = c * share_a, BEHIND[0] + c * share_b
    y_ahead = Ring(wires, ybuf, "track", ny, *AHEAD)
    y_behind = Ring(wires, ybuf, "track", ny, *BEHIND)
    c_ahead = Ring(wires, cbuf, "tm_2", nc, *AHEAD)
    c_behind = Ring(wires, cbuf, "tm_2", nc, *BEHIND)
    x_ahead = Ring(wires, xbuf, "tm_1", nx, own_a, share_a)
    x_behind = Ring(wires, xbuf, "tm_1", nx, own_b, share_b)
    fill(stree, compose_ahead)
    ybuf[y, pl.ds(0, ROWS)] = stree[-1][0][pl.ds(0, ROWS)]
    g_move.relay()
    y_ahead.start()
    g_move.finish(g_own)
    y_ahead.relay()

    us, ps = backward_pass(g_own, x_all, e_all, hi_ref, lo_ref, s_all)
    for seg in range(SEGS):
        segs[seg, pl.ds(W_MAT, ROWS)] = us[seg]
        segs[seg, pl.ds(PSI, N)] = ps[seg]
    fill(stree, compose_behind)
    ybuf[y, pl.ds(W_MAT, ROWS + N)] = stree[-1][0][pl.ds(W_MAT, ROWS + N)]
    y_behind.start()

    def share_start(own, share):
        rows = pl.ds(pl.multiple_of(own, 8), share)
        parts = [xbuf.at[lax.rem(x + step, nx), rows] for step in range(1, nx)] if nc > 1 else []
        return [wires.go(part, part, tm_2=1 - c) for part in parts]

    def to_slabs(buf, rows, later):
        mine = pl.ds(pl.multiple_of(c * (rows // nc), 8), rows // nc)
        part = buf.at[z, mine]
        moves = []
        for step in range(1, nz):
            there = z + step if later else z - step
            copy = wires.make(part, part, tm_0=jnp.clip(there, 0, nz - 1))
            use = there < nz if later else jnp.logical_and(there >= 0, z < nz - 1)
            moves.append((copy, use))
            pl.when(use)(copy.start)
        return mine, moves

    def from_slabs(buf, mine, moves, later):
        shared = []
        for step, (copy, _) in enumerate(moves, 1):
            source = z - step if later else z + step
            use = source >= 0 if later else source < nz - 1
            pl.when(use)(copy.wait_recv)
            if nc > 1:
                part = buf.at[jnp.clip(source, 0, nz - 1), mine]
                over = wires.make(part, part, tm_2=1 - c)
                pl.when(use)(over.start)
                shared.append((over, use))
        for copy, use in shared:
            pl.when(use)(copy.wait_recv)
        for copy, use in moves + shared:
            pl.when(use)(copy.wait_send)

    y_ahead.finish()
    fill(ytree, compose_ahead)
    cbuf[c, pl.ds(0, ROWS)] = ytree[-1][0][pl.ds(0, ROWS)]
    c_ahead.start()
    c_ahead.finish()
    fill(ctree, compose_ahead)
    xbuf[x, pl.ds(0, ROWS)] = ctree[-1][0][pl.ds(0, ROWS)]
    x_ahead.start()
    y_behind.relay()
    x_ahead.relay()
    y_behind.finish()
    fill(ytree, compose_behind)
    cbuf[c, pl.ds(W_MAT, ROWS + N)] = ytree[-1][0][pl.ds(W_MAT, ROWS + N)]
    c_behind.start()
    x_ahead.finish()
    shared = share_start(own_a, share_a)
    c_behind.finish()
    fill(ctree, compose_behind)
    xbuf[x, pl.ds(W_MAT, ROWS + N)] = ctree[-1][0][pl.ds(W_MAT, ROWS + N)]
    x_behind.start()
    for copy in shared:
        copy.wait_recv()
    fill(xtree, compose_ahead)
    total = xtree[-1][0]
    zpv[z] = total[pl.ds(0, ROWS)]
    z_ahead = to_slabs(zpv, ROWS, True)
    x_behind.relay()
    x_behind.finish()
    for copy in share_start(own_b, share_b):
        copy.wait_recv()
    fill(xtree, compose_psi)
    zps[z] = total[pl.ds(PSI, N)]
    z_behind = to_slabs(zps, N, False)
    from_slabs(zpv, *z_ahead, True)

    zero = jnp.zeros((TR, N), F32)
    entering, state = zero, zero
    for i in range(nz - 1):
        got = jnp.minimum(i, z)
        after = zpv[got, pl.ds(V_ROW, TR)]
        if i > 0:
            after = after + product(state, zpv[got, pl.ds(PHI, N)])
        state = after
        entering = jnp.where(z == i + 1, state, entering)
    chip_x = [entering]
    for i in range(nx - 1):
        chip_x.append(middle_x(chip_x[-1], xbuf.at[i]))
    chip_w = [product(chip_x[i], xbuf[i, pl.ds(W_MAT, N)]) + xbuf[i, pl.ds(W_ROW, TR)] for i in range(nx)]

    def leave_chips(state):
        states = [state]
        for i in range(nx - 1, -1, -1):
            states.append(chip_w[i] if states[-1] is None else product(states[-1], xbuf[i, pl.ds(PSI, N)]) + chip_w[i])
        return states[::-1]

    zc[z] = leave_chips(None)[0]
    part = zc.at[z]
    group = [wires.go(part, part, tm_0=lax.rem(z + step, nz)) for step in range(1, nz)]
    from_slabs(zps, *z_behind, False)
    for copy in group:
        copy.wait_recv()
    leaving, state = zero, zero
    for i in range(nz - 1, 0, -1):
        after = zc[i]
        if i < nz - 1:
            after = after + product(state, zps[jnp.maximum(i, z)])
        state = after
        leaving = jnp.where(z == i - 1, state, leaving)

    chip_u = leave_chips(leaving)
    xv, uv = chip_x[0], chip_u[1]
    for i in range(1, nx):
        xv, uv = jnp.where(x == i, chip_x[i], xv), jnp.where(x == i, chip_u[i + 1], uv)
    xv, uv = descend(xv, uv, ctree, c)
    xv, uv = descend(xv, uv, ytree, y)

    homes, detours = [], []

    def target(first, count):
        return out_ref.at[pl.ds(pl.multiple_of(y * each + first, 8), count)]

    def sent(first, count):
        rows = pl.ds(first, count)
        if first < half:
            detours.append((wires.go(out_buf.at[far, rows], o_way.at[1, rows], track=left), rows, first, count))
        for there in (right, left) if first < half else others:
            homes.append(wires.go(out_buf.at[there, rows], target(first, count), track=there))

    final_pass(xv, uv, stree, hi_ref, lo_ref, s_all, out_buf, sent)
    out_ref[own_rows] = out_buf[y]
    for copy, rows, first, count in detours:
        copy.wait_recv()
        there = out_ref.at[pl.ds(pl.multiple_of(right * each + first, 8), count)]
        homes.append(wires.go(o_way.at[1, rows], there, track=left))
    for copy in homes:
        copy.wait_recv()
    wires.close()


def main_call(sizes, ids, dyn, smooth, gain, obs):
    ny, nz, nx, nc = sizes
    count, owned = ids.shape[0], dyn.shape[0]
    blocks = count // ny
    each = obs.shape[0] // ny
    steps = each // (TR // ny)
    links = 20 + 30 + 2 * (1 + nx) + 5 * nz + 3 * SEGS
    hbm = pl.BlockSpec(memory_space=pltpu.MemorySpace.HBM)
    vmem = pl.BlockSpec(memory_space=VMEM)
    return pl.pallas_call(
        functools.partial(main_kernel, sizes),
        out_shape=jax.ShapeDtypeStruct(obs.shape, F32),
        in_specs=[pl.BlockSpec(memory_space=pltpu.MemorySpace.SMEM), hbm, hbm, hbm, hbm],
        out_specs=vmem,
        scratch_shapes=[
            pltpu.VMEM((owned, N, N), BF16),
            pltpu.VMEM((owned, N, N), BF16),
            pltpu.VMEM((owned, N), BF16),
            pltpu.VMEM((owned, N), F32),
            pltpu.VMEM((count, N, N), BF16),
            pltpu.VMEM((count, N, N), BF16),
            pltpu.VMEM((count, N), F32),
            pltpu.SemaphoreType.DMA((4,)),
            pltpu.VMEM((2, 4, blocks // 2, N, N), BF16),
            pltpu.VMEM((2, 2, blocks, N, N), BF16),
            pltpu.VMEM((4, blocks, N), F32),
            pltpu.VMEM((4, each, N), F32),
            pltpu.VMEM((2, each // 2, N), F32),
            pltpu.VMEM((blocks, N, N), BF16),
            pltpu.VMEM((blocks, N, N), BF16),
            pltpu.VMEM((blocks, N), F32),
            pltpu.VMEM((steps, TR, N), F32),
            pltpu.VMEM((steps, ROWS, N), F32),
            pltpu.VMEM((steps, ROWS, N), F32),
            pltpu.VMEM((steps, 2 * N, N), BF16),
            pltpu.VMEM((steps, 2 * N, N), BF16),
            pltpu.VMEM((steps, TR, N), F32),
            pltpu.VMEM((SEGS, MAP, N), F32),
            pltpu.VMEM((SEGS - 1, MAP, N), F32),
            pltpu.VMEM((ny, MAP, N), F32),
            pltpu.VMEM((max(ny - 1, 1), MAP, N), F32),
            pltpu.VMEM((nc, MAP, N), F32),
            pltpu.VMEM((max(nc - 1, 1), MAP, N), F32),
            pltpu.VMEM((nx, MAP, N), F32),
            pltpu.VMEM((max(nx - 1, 1), MAP, N), F32),
            pltpu.VMEM((nz, ROWS, N), F32),
            pltpu.VMEM((nz, N, N), F32),
            pltpu.VMEM((nz, TR, N), F32),
            pltpu.VMEM((4, each, N), F32),
            pltpu.SemaphoreType.DMA((links,)),
            pltpu.SemaphoreType.DMA((links,)),
        ],
        compiler_params=pltpu.CompilerParams(
            collective_id=1, has_side_effects=True, vmem_limit_bytes=67043328
        ),
        name="smooth",
    )(ids, dyn, smooth, gain, obs)


def body(sizes, observations, dynamics, smoother_gain, gains, regime):
    out = main_call(sizes, regime, dynamics, smoother_gain, gains, observations.reshape(-1, N))
    return out.reshape(observations.shape)


def build(torus):
    sizes = tuple(torus.shape[a] for a in ("track",) + TM)
    placed = (
        P(TM, "track", None),
        P("track", None, None),
        P("track", None, None),
        P("track", None),
        P(TM),
    )
    return jax.shard_map(
        functools.partial(body, sizes),
        mesh=torus,
        in_specs=placed,
        out_specs=P(TM, "track", None),
        check_vma=False,
    )


def solution(mesh):
    return build(Mesh(mesh.devices.reshape(mesh.shape["track"], 8, 4, 2), ("track",) + TM))
```

```python
import functools

import jax
import jax.numpy as jnp
import numpy as np
from jax import lax
from jax.experimental import pallas as pl
from jax.experimental.pallas import tpu as pltpu
from jax.sharding import Mesh
from jax.sharding import PartitionSpec as P

TM = ("tm_0", "tm_1", "tm_2")
F32 = jnp.float32
BF16 = jnp.bfloat16
N = 128
TR = 16
ROWS = N + TR
MAP = 2 * ROWS + N
SEGS = 4
MESH = pl.DeviceIdType.MESH
VMEM = pltpu.MemorySpace.VMEM


def split2(x):
    hi = x.astype(BF16)
    return hi, (x - hi.astype(F32)).astype(BF16)


def split3(x):
    hi = x.astype(BF16)
    rest = x - hi.astype(F32)
    mid = rest.astype(BF16)
    return hi, mid, (rest - mid.astype(F32)).astype(BF16)


def dot_t(left, right):
    return lax.dot_general(left, right, (((1,), (1,)), ((), ())), preferred_element_type=F32)


def times_t(x, w):
    hi, mid, low = split3(x)
    return dot_t(jnp.concatenate([hi, mid], axis=1), jnp.concatenate([w, w], axis=1)) + dot_t(low, w)


def product(x, w):
    xh, xl = split2(x)
    wh, wl = split2(w)
    return jnp.dot(
        jnp.concatenate([xh, xl, xh], axis=1),
        jnp.concatenate([wh, wh, wl], axis=0),
        preferred_element_type=F32,
    )


PHI, V_ROW, W_MAT, W_ROW, PSI = 0, N, ROWS, ROWS + N, 2 * ROWS
AHEAD, BEHIND = (0, ROWS), (ROWS, MAP - ROWS)


def compose_ahead(left, right, out):
    both = product(left[pl.ds(0, ROWS)], right[pl.ds(PHI, N)])
    out[pl.ds(0, N)] = both[:N]
    out[pl.ds(V_ROW, TR)] = both[N:] + right[pl.ds(V_ROW, TR)]


def compose_behind(left, right, out):
    both = product(left[pl.ds(0, ROWS)], right[pl.ds(W_MAT, N)])
    last = both[N:] + right[pl.ds(W_ROW, TR)]
    back = product(jnp.concatenate([both[:N], last, right[pl.ds(PSI, N)]], axis=0), left[pl.ds(PSI, N)])
    out[pl.ds(W_MAT, ROWS)] = back[:ROWS] + left[pl.ds(W_MAT, ROWS)]
    out[pl.ds(PSI, N)] = back[ROWS:]


def middle_x(x, left):
    return product(x, left[pl.ds(PHI, N)]) + left[pl.ds(V_ROW, TR)]


def tree_of(leaves, nodes):
    levels, used = [leaves], 0
    while len(levels[-1]) > 1:
        row = [nodes.at[used + i] for i in range(len(levels[-1]) // 2)]
        used += len(row)
        levels.append(row)
    return levels


def fill(levels, compose):
    for below, row in zip(levels, levels[1:]):
        for i, node in enumerate(row):
            compose(below[2 * i], below[2 * i + 1], node)


def cross(x_mid, right):
    return product(x_mid, right[pl.ds(W_MAT, N)]) + right[pl.ds(W_ROW, TR)]


def descend_x(x, levels, position):
    plan = []
    for level in range(len(levels) - 2, -1, -1):
        row = levels[level]
        bit = lax.rem(lax.div(position, 2**level), 2)
        above = lax.div(position, 2 ** (level + 1))
        best, terms = None, []
        for i in range(len(row) // 2):
            x_mid = middle_x(x, row[2 * i])
            terms.append((row[2 * i + 1], cross(x_mid, row[2 * i + 1])))
            best = x_mid if best is None else jnp.where(above == i, x_mid, best)
        plan.append((bit, above, terms))
        x = jnp.where(bit == 1, best, x)
    return x, plan


def descend_u(u, plan):
    for bit, above, terms in plan:
        best = None
        for i, (right, term) in enumerate(terms):
            u_mid = product(u, right[pl.ds(PSI, N)]) + term
            best = u_mid if best is None else jnp.where(above == i, u_mid, best)
        u = jnp.where(bit == 1, u, best)
    return u


class Wires:
    def __init__(self, send, recv):
        self.send, self.recv, self.used = send, recv, 0
        self.pending = []

    def make(self, src, dst, **peer):
        copy = pltpu.make_async_remote_copy(
            src_ref=src,
            dst_ref=dst,
            send_sem=self.send.at[self.used],
            recv_sem=self.recv.at[self.used],
            device_id=peer,
            device_id_type=MESH,
        )
        self.used += 1
        return copy

    def go(self, src, dst, **peer):
        copy = self.make(src, dst, **peer)
        copy.start()
        self.pending.append(copy)
        return copy

    def close(self):
        for copy in self.pending:
            copy.wait_send()


def compose_psi(left, right, out):
    out[pl.ds(PSI, N)] = product(right[pl.ds(PSI, N)], left[pl.ds(PSI, N)])


class Ring:
    def __init__(self, wires, buf, axis, size, first, count):
        self.wires, self.buf, self.axis, self.size = wires, buf, axis, size
        self.me = lax.axis_index(axis)
        half = -(-count // 16) * 8
        self.rows = [pl.ds(first, count)]
        if size > 2:
            self.rows = [
                pl.ds(pl.multiple_of(first, 8), half),
                pl.ds(pl.multiple_of(first + half, 8), count - half),
            ]

    def send(self, who, part, there):
        piece = self.buf.at[who, self.rows[part]]
        return self.wires.go(piece, piece, **{self.axis: there})

    def start(self):
        if self.size == 2:
            self.rest = [self.send(self.me, 0, 1 - self.me)]
        if self.size > 2:
            self.right = lax.rem(self.me + 1, self.size)
            self.left = lax.rem(self.me + self.size - 1, self.size)
            self.first = [self.send(self.me, 0, self.right), self.send(self.me, 1, self.left)]
            self.rest = [self.send(self.me, 1, self.right), self.send(self.me, 0, self.left)]

    def relay(self):
        if self.size > 2:
            self.first[0].wait_recv()
            self.rest.append(self.send(self.left, 0, self.right))
            self.first[1].wait_recv()
            self.rest.append(self.send(self.right, 1, self.left))

    def finish(self):
        if self.size > 1:
            for copy in self.rest:
                copy.wait_recv()


class Merge:
    def __init__(self, wires, cand, relay, arrived, y):
        self.wires, self.cand, self.relay_buf, self.arrived, self.y = wires, cand, relay, arrived, y
        self.right, self.left, self.far = (lax.rem(y + k, 4) for k in (1, 3, 2))
        self.each = cand.shape[0] // 4
        self.half = self.each // 2

    def part(self, owner, side):
        return pl.ds(owner * self.each + side * self.half, self.half)

    def start(self):
        go, cand, half = self.wires.go, self.cand, self.half
        low, high = pl.ds(0, half), pl.ds(half, half)
        self.via = [
            go(cand.at[self.part(self.far, 0)], self.relay_buf.at[0], track=self.right),
            go(cand.at[self.part(self.far, 1)], self.relay_buf.at[1], track=self.left),
        ]
        self.rest = [
            go(cand.at[self.part(self.right, 1)], self.arrived.at[0, high], track=self.right),
            go(cand.at[self.part(self.left, 0)], self.arrived.at[1, low], track=self.left),
        ]

    def relay(self):
        go, half = self.wires.go, self.half
        for side, (there, rows) in enumerate(((self.right, pl.ds(0, half)), (self.left, pl.ds(half, half)))):
            self.via[side].wait_recv()
            self.relay_buf[2 + side] = self.relay_buf[side] + self.cand[self.part(there, side)]
            self.rest.append(go(self.relay_buf.at[2 + side], self.arrived.at[side, rows], track=there))

    def finish(self, out):
        for copy in self.rest:
            copy.wait_recv()
        out[...] = self.cand[pl.ds(self.y * self.each, self.each)] + (self.arrived[0] + self.arrived[1])


def forward_pass(a_own, k_own, o_all, x_all, e_all):
    count = a_own.shape[0]
    dwell = o_all.shape[0] // count
    per = count // SEGS
    eye = (
        lax.broadcasted_iota(jnp.int32, (N, N), 0) == lax.broadcasted_iota(jnp.int32, (N, N), 1)
    ).astype(F32)
    start = jnp.concatenate([eye, jnp.zeros((TR, N), F32)], axis=0)
    blank = jnp.zeros((N, N), F32)

    def some(i, xs):
        new_x = list(xs)
        for step in range(dwell):
            for seg in range(SEGS):
                block = seg * per + i
                t = block * dwell + step
                pred = times_t(new_x[seg], a_own[block])
                obs = jnp.concatenate([blank, o_all[t]], axis=0)
                e = k_own[pl.ds(block, 1)] * (obs - pred)
                e_all[t] = e
                x_all[t] = pred + e
                new_x[seg] = pred + e
        return tuple(new_x)

    return lax.fori_loop(0, per, some, (start,) * SEGS)


def backward_pass(g_own, x_all, e_all, hi_ref, lo_ref, s_all, between):
    count = g_own.shape[0]
    dwell = x_all.shape[0] // count
    per = count // SEGS
    eye = (
        lax.broadcasted_iota(jnp.int32, (N, N), 0) == lax.broadcasted_iota(jnp.int32, (N, N), 1)
    ).astype(F32)

    def keep(t, row, value):
        hi, low = split2(value)
        hi_ref[t, pl.ds(row, N)] = hi
        lo_ref[t, pl.ds(row, N)] = low

    def some(i, carry):
        new_u, new_p = list(carry[0]), list(carry[1])
        for step in range(dwell):
            for seg in range(SEGS):
                block = seg * per + per - 1 - i
                t = block * dwell + dwell - 1 - step
                s = x_all[t] + new_u[seg]
                keep(t, 0, s[:N])
                keep(t, N, new_p[seg])
                s_all[t] = s[N:]
                back = times_t(jnp.concatenate([new_u[seg] + e_all[t], new_p[seg]], axis=0), g_own[block])
                new_u[seg], new_p[seg] = back[:ROWS], back[ROWS:]
        return tuple(new_u), tuple(new_p)

    carry = lax.fori_loop(0, per // 2, some, ((jnp.zeros((ROWS, N), F32),) * SEGS, (eye,) * SEGS))
    between()
    return lax.fori_loop(per // 2, per, some, carry)


def response(state, hi_ref, lo_ref, t, row):
    hi, low = split2(state)
    first = jnp.dot(jnp.concatenate([hi, low], axis=0), hi_ref[t, pl.ds(row, N)], preferred_element_type=F32)
    return (first[:TR] + first[TR:]) + jnp.dot(hi, lo_ref[t, pl.ds(row, N)], preferred_element_type=F32)


def final_x(x, levels, hi_ref, lo_ref, s_all):
    xs, plan = [x], []
    for row in levels[-2::-1]:
        new, terms = [], []
        for i, x in enumerate(xs):
            x_mid = middle_x(x, row[2 * i])
            new += [x, x_mid]
            terms.append((row[2 * i + 1], cross(x_mid, row[2 * i + 1])))
        xs = new
        plan.append(terms)
    per = s_all.shape[0] // SEGS
    for seg, x in enumerate(xs):
        for t in range(seg * per, seg * per + per):
            s_all[t] = s_all[t] + response(x, hi_ref, lo_ref, t, 0)
    return plan


def final_u(u, plan, hi_ref, lo_ref, s_all, out_buf, sent):
    us = [u]
    for terms in plan:
        new = []
        for u, (right, term) in zip(us, terms):
            new += [product(u, right[pl.ds(PSI, N)]) + term, u]
        us = new
    per = s_all.shape[0] // SEGS
    four = TR // 4
    for seg, u in enumerate(us):
        for pair in range(per // 2):
            first = seg * per + 2 * pair
            outs = [s_all[t] + response(u, hi_ref, lo_ref, t, N) for t in (first, first + 1)]
            for group in range(4):
                rows = slice(four * group, four * group + four)
                out_buf[group, pl.ds(first * four, 2 * four)] = jnp.concatenate(
                    [outs[0][rows], outs[1][rows]], axis=0
                )
        sent(seg * per * four, per * four)


def main_kernel(sizes, *refs):
    (ids, dyn, smooth, gain, obs_in, out_ref, tab_a, tab_g, tab_s, tab_k, ca, cg, ck, local, relay, arrived, k_buf, o_buf, o_way, a_own, g_own, k_own, o_all, x_all, e_all,
     hi_ref, lo_ref, s_all, segs, segnode, ybuf, ynode, cbuf, cnode, xbuf, xnode, zpv, zps, zc, out_buf,
     send, recv) = refs
    ny, nz, nx, nc = sizes
    y, z, x, c = (lax.axis_index(a) for a in ("track",) + TM)
    each = obs_in.shape[0] // 4
    blocks = a_own.shape[0]
    own_rows = pl.ds(pl.multiple_of(y * each, each), each)
    fetch_a = pltpu.make_async_copy(dyn, tab_a, local.at[0])
    fetch_g = pltpu.make_async_copy(smooth, tab_g, local.at[1])
    fetch_o = pltpu.make_async_copy(obs_in.at[own_rows], o_buf.at[y], local.at[2])
    fetch_k = pltpu.make_async_copy(gain, tab_s, local.at[3])
    for copy in (fetch_k, fetch_a, fetch_g, fetch_o):
        copy.start()
    barrier = pltpu.get_barrier_semaphore()
    peers = []
    for axis, me, size in (("track", y, ny), ("tm_0", z, nz), ("tm_1", x, nx), ("tm_2", c, nc)):
        for step in range(1, size):
            peers.append({axis: lax.rem(me + step, size)})
    for peer in peers:
        pl.semaphore_signal(barrier, inc=1, device_id=peer, device_id_type=MESH)
    fetch_k.wait()
    tab_k[...] = tab_s[...].astype(F32)
    owned = tab_a.shape[0]
    zero_mat = jnp.zeros((N, N), BF16)

    def picked(b):
        row = ids[b] - y * owned
        return jnp.logical_and(row >= 0, row < owned), jnp.clip(row, 0, owned - 1)

    def pick_a(b, _):
        here, row = picked(b)
        ca[b] = jnp.where(here, tab_a[row], zero_mat)
        ck[pl.ds(b, 1)] = jnp.where(here, tab_k[pl.ds(row, 1)], 0.0)
        return 0

    def pick_g(b, _):
        here, row = picked(b)
        cg[b] = jnp.where(here, tab_g[row], zero_mat)
        return 0

    fetch_a.wait()
    lax.fori_loop(0, ca.shape[0], pick_a, 0)
    pl.semaphore_wait(barrier, len(peers))
    wires = Wires(send, recv)
    right, left, far = others = [lax.rem(y + k, 4) for k in (1, 3, 2)]

    a_move = Merge(wires, ca, relay.at[0], arrived.at[0], y)
    g_move = Merge(wires, cg, relay.at[1], arrived.at[1], y)
    a_move.start()
    small = []
    half = each // 2

    def obs_rows(owner, first, count):
        return obs_in.at[pl.ds(pl.multiple_of(owner * each + first, 8), count)]

    for there in (right, left):
        small.append(wires.go(obs_rows(there, 0, each), o_buf.at[y], track=there))
    small.append(wires.go(obs_rows(far, 0, half), o_buf.at[y, pl.ds(0, half)], track=far))
    detour = wires.go(obs_rows(far, half, half), o_way.at[0], track=left)
    for there in others:
        small.append(wires.go(ck.at[pl.ds(pl.multiple_of(there * blocks, blocks), blocks)], k_buf.at[y], track=there))
    k_buf[y] = ck[pl.ds(pl.multiple_of(y * blocks, blocks), blocks)]
    fetch_g.wait()
    lax.fori_loop(0, cg.shape[0], pick_g, 0)
    a_move.relay()
    detour.wait_recv()
    small.append(wires.go(o_way.at[0], o_buf.at[right, pl.ds(half, half)], track=left))
    g_move.start()
    a_move.finish(a_own)
    for copy in small:
        copy.wait_recv()
    fetch_o.wait()
    k_own[...] = (k_buf[0] + k_buf[1]) + (k_buf[2] + k_buf[3])
    four = TR // 4

    def in_steps(p, _):
        tiles = [o_buf[s, pl.ds(pl.multiple_of(p * 2 * four, 8), 2 * four)] for s in range(4)]
        o_all[2 * p] = jnp.concatenate([tile[:four] for tile in tiles], axis=0)
        o_all[2 * p + 1] = jnp.concatenate([tile[four:] for tile in tiles], axis=0)
        return 0

    lax.fori_loop(0, each // (2 * four), in_steps, 0)

    xs = forward_pass(a_own, k_own, o_all, x_all, e_all)
    for seg in range(SEGS):
        segs[seg, pl.ds(0, ROWS)] = xs[seg]
    stree = tree_of([segs.at[i] for i in range(SEGS)], segnode)
    ytree = tree_of([ybuf.at[i] for i in range(ny)], ynode)
    ctree = tree_of([cbuf.at[i] for i in range(nc)], cnode)
    xtree = tree_of([xbuf.at[i] for i in range(nx)], xnode)
    share_a, share_b = AHEAD[1] // nc, BEHIND[1] // nc
    own_a, own_b = c * share_a, BEHIND[0] + c * share_b
    y_ahead = Ring(wires, ybuf, "track", ny, *AHEAD)
    y_behind = Ring(wires, ybuf, "track", ny, *BEHIND)
    c_ahead = Ring(wires, cbuf, "tm_2", nc, *AHEAD)
    c_behind = Ring(wires, cbuf, "tm_2", nc, *BEHIND)
    x_ahead = Ring(wires, xbuf, "tm_1", nx, own_a, share_a)
    x_behind = Ring(wires, xbuf, "tm_1", nx, own_b, share_b)
    fill(stree, compose_ahead)
    ybuf[y, pl.ds(0, ROWS)] = stree[-1][0][pl.ds(0, ROWS)]
    g_move.relay()
    y_ahead.start()
    g_move.finish(g_own)

    us, ps = backward_pass(g_own, x_all, e_all, hi_ref, lo_ref, s_all, y_ahead.relay)
    for seg in range(SEGS):
        segs[seg, pl.ds(W_MAT, ROWS)] = us[seg]
        segs[seg, pl.ds(PSI, N)] = ps[seg]
    fill(stree, compose_behind)
    ybuf[y, pl.ds(W_MAT, ROWS + N)] = stree[-1][0][pl.ds(W_MAT, ROWS + N)]
    y_behind.start()

    def share_start(own, share):
        rows = pl.ds(pl.multiple_of(own, 8), share)
        parts = [xbuf.at[lax.rem(x + step, nx), rows] for step in range(1, nx)] if nc > 1 else []
        return [wires.go(part, part, tm_2=1 - c) for part in parts]

    def to_slabs(buf, rows, later):
        mine = pl.ds(pl.multiple_of(c * (rows // nc), 8), rows // nc)
        part = buf.at[z, mine]
        moves = []
        for step in range(1, nz):
            there = z + step if later else z - step
            copy = wires.make(part, part, tm_0=jnp.clip(there, 0, nz - 1))
            use = there < nz if later else jnp.logical_and(there >= 0, z < nz - 1)
            moves.append((copy, use))
            pl.when(use)(copy.start)
        return mine, moves

    def from_slabs(buf, mine, moves, later):
        shared = []
        for step, (copy, _) in enumerate(moves, 1):
            source = z - step if later else z + step
            use = source >= 0 if later else source < nz - 1
            pl.when(use)(copy.wait_recv)
            if nc > 1:
                part = buf.at[jnp.clip(source, 0, nz - 1), mine]
                over = wires.make(part, part, tm_2=1 - c)
                pl.when(use)(over.start)
                shared.append((over, use))
        for copy, use in shared:
            pl.when(use)(copy.wait_recv)
        for copy, use in moves + shared:
            pl.when(use)(copy.wait_send)

    y_ahead.finish()
    fill(ytree, compose_ahead)
    cbuf[c, pl.ds(0, ROWS)] = ytree[-1][0][pl.ds(0, ROWS)]
    c_ahead.start()
    c_ahead.finish()
    fill(ctree, compose_ahead)
    xbuf[x, pl.ds(0, ROWS)] = ctree[-1][0][pl.ds(0, ROWS)]
    x_ahead.start()
    y_behind.relay()
    x_ahead.relay()
    y_behind.finish()
    fill(ytree, compose_behind)
    cbuf[c, pl.ds(W_MAT, ROWS + N)] = ytree[-1][0][pl.ds(W_MAT, ROWS + N)]
    c_behind.start()
    x_ahead.finish()
    shared = share_start(own_a, share_a)
    c_behind.finish()
    fill(ctree, compose_behind)
    xbuf[x, pl.ds(W_MAT, ROWS + N)] = ctree[-1][0][pl.ds(W_MAT, ROWS + N)]
    x_behind.start()
    for copy in shared:
        copy.wait_recv()
    fill(xtree, compose_ahead)
    total = xtree[-1][0]
    zpv[z] = total[pl.ds(0, ROWS)]
    z_ahead = to_slabs(zpv, ROWS, True)
    x_behind.relay()
    x_behind.finish()
    for copy in share_start(own_b, share_b):
        copy.wait_recv()
    fill(xtree, compose_psi)
    zps[z] = total[pl.ds(PSI, N)]
    z_behind = to_slabs(zps, N, False)
    from_slabs(zpv, *z_ahead, True)

    zero = jnp.zeros((TR, N), F32)
    entering, state = zero, zero
    for i in range(nz - 1):
        got = jnp.minimum(i, z)
        after = zpv[got, pl.ds(V_ROW, TR)]
        if i > 0:
            after = after + product(state, zpv[got, pl.ds(PHI, N)])
        state = after
        entering = jnp.where(z == i + 1, state, entering)
    chip_x = [entering]
    for i in range(nx - 1):
        chip_x.append(middle_x(chip_x[-1], xbuf.at[i]))
    chip_w = [product(chip_x[i], xbuf[i, pl.ds(W_MAT, N)]) + xbuf[i, pl.ds(W_ROW, TR)] for i in range(nx)]

    def leave_chips(state):
        states = [state]
        for i in range(nx - 1, -1, -1):
            states.append(chip_w[i] if states[-1] is None else product(states[-1], xbuf[i, pl.ds(PSI, N)]) + chip_w[i])
        return states[::-1]

    zc[z] = leave_chips(None)[0]
    part = zc.at[z]
    group = [wires.go(part, part, tm_0=lax.rem(z + step, nz)) for step in range(1, nz)]
    xv = chip_x[0]
    for i in range(1, nx):
        xv = jnp.where(x == i, chip_x[i], xv)
    xv, c_plan = descend_x(xv, ctree, c)
    xv, y_plan = descend_x(xv, ytree, y)
    s_plan = final_x(xv, stree, hi_ref, lo_ref, s_all)
    from_slabs(zps, *z_behind, False)
    for copy in group:
        copy.wait_recv()
    leaving, state = zero, zero
    for i in range(nz - 1, 0, -1):
        after = zc[i]
        if i < nz - 1:
            after = after + product(state, zps[jnp.maximum(i, z)])
        state = after
        leaving = jnp.where(z == i - 1, state, leaving)

    chip_u = leave_chips(leaving)
    uv = chip_u[1]
    for i in range(1, nx):
        uv = jnp.where(x == i, chip_u[i + 1], uv)
    uv = descend_u(descend_u(uv, c_plan), y_plan)

    homes, detours = [], []

    def target(first, count):
        return out_ref.at[pl.ds(pl.multiple_of(y * each + first, 8), count)]

    def sent(first, count):
        rows = pl.ds(first, count)
        if first < half:
            detours.append((wires.go(out_buf.at[far, rows], o_way.at[1, rows], track=left), rows, first, count))
        for there in (right, left) if first < half else others:
            homes.append(wires.go(out_buf.at[there, rows], target(first, count), track=there))

    final_u(uv, s_plan, hi_ref, lo_ref, s_all, out_buf, sent)
    out_ref[own_rows] = out_buf[y]
    for copy, rows, first, count in detours:
        copy.wait_recv()
        there = out_ref.at[pl.ds(pl.multiple_of(right * each + first, 8), count)]
        homes.append(wires.go(o_way.at[1, rows], there, track=left))
    for copy in homes:
        copy.wait_recv()
    wires.close()


def main_call(sizes, ids, dyn, smooth, gain, obs):
    ny, nz, nx, nc = sizes
    count, owned = ids.shape[0], dyn.shape[0]
    blocks = count // ny
    each = obs.shape[0] // ny
    steps = each // (TR // ny)
    links = 20 + 30 + 2 * (1 + nx) + 5 * nz + 3 * SEGS
    hbm = pl.BlockSpec(memory_space=pltpu.MemorySpace.HBM)
    vmem = pl.BlockSpec(memory_space=VMEM)
    return pl.pallas_call(
        functools.partial(main_kernel, sizes),
        out_shape=jax.ShapeDtypeStruct(obs.shape, F32),
        in_specs=[pl.BlockSpec(memory_space=pltpu.MemorySpace.SMEM), hbm, hbm, hbm, hbm],
        out_specs=vmem,
        scratch_shapes=[
            pltpu.VMEM((owned, N, N), BF16),
            pltpu.VMEM((owned, N, N), BF16),
            pltpu.VMEM((owned, N), BF16),
            pltpu.VMEM((owned, N), F32),
            pltpu.VMEM((count, N, N), BF16),
            pltpu.VMEM((count, N, N), BF16),
            pltpu.VMEM((count, N), F32),
            pltpu.SemaphoreType.DMA((4,)),
            pltpu.VMEM((2, 4, blocks // 2, N, N), BF16),
            pltpu.VMEM((2, 2, blocks, N, N), BF16),
            pltpu.VMEM((4, blocks, N), F32),
            pltpu.VMEM((4, each, N), F32),
            pltpu.VMEM((2, each // 2, N), F32),
            pltpu.VMEM((blocks, N, N), BF16),
            pltpu.VMEM((blocks, N, N), BF16),
            pltpu.VMEM((blocks, N), F32),
            pltpu.VMEM((steps, TR, N), F32),
            pltpu.VMEM((steps, ROWS, N), F32),
            pltpu.VMEM((steps, ROWS, N), F32),
            pltpu.VMEM((steps, 2 * N, N), BF16),
            pltpu.VMEM((steps, 2 * N, N), BF16),
            pltpu.VMEM((steps, TR, N), F32),
            pltpu.VMEM((SEGS, MAP, N), F32),
            pltpu.VMEM((SEGS - 1, MAP, N), F32),
            pltpu.VMEM((ny, MAP, N), F32),
            pltpu.VMEM((max(ny - 1, 1), MAP, N), F32),
            pltpu.VMEM((nc, MAP, N), F32),
            pltpu.VMEM((max(nc - 1, 1), MAP, N), F32),
            pltpu.VMEM((nx, MAP, N), F32),
            pltpu.VMEM((max(nx - 1, 1), MAP, N), F32),
            pltpu.VMEM((nz, ROWS, N), F32),
            pltpu.VMEM((nz, N, N), F32),
            pltpu.VMEM((nz, TR, N), F32),
            pltpu.VMEM((4, each, N), F32),
            pltpu.SemaphoreType.DMA((links,)),
            pltpu.SemaphoreType.DMA((links,)),
        ],
        compiler_params=pltpu.CompilerParams(
            collective_id=1, has_side_effects=True, vmem_limit_bytes=67043328
        ),
        name="smooth",
    )(ids, dyn, smooth, gain, obs)


def body(sizes, observations, dynamics, smoother_gain, gains, regime):
    out = main_call(sizes, regime, dynamics, smoother_gain, gains, observations.reshape(-1, N))
    return out.reshape(observations.shape)


def build(torus):
    sizes = tuple(torus.shape[a] for a in ("track",) + TM)
    placed = (
        P(TM, "track", None),
        P("track", None, None),
        P("track", None, None),
        P("track", None),
        P(TM),
    )
    return jax.shard_map(
        functools.partial(body, sizes),
        mesh=torus,
        in_specs=placed,
        out_specs=P(TM, "track", None),
        check_vma=False,
    )


def solution(mesh):
    return build(Mesh(mesh.devices.reshape(mesh.shape["track"], 8, 4, 2), ("track",) + TM))
```

```python
import functools

import jax
import jax.numpy as jnp
import numpy as np
from jax import lax
from jax.experimental import pallas as pl
from jax.experimental.pallas import tpu as pltpu
from jax.sharding import Mesh
from jax.sharding import PartitionSpec as P

TM = ("tm_0", "tm_1", "tm_2")
F32 = jnp.float32
BF16 = jnp.bfloat16
N = 128
TR = 16
ROWS = N + TR
MAP = 2 * ROWS + N
SEGS = 4
MESH = pl.DeviceIdType.MESH
VMEM = pltpu.MemorySpace.VMEM


def split2(x):
    hi = x.astype(BF16)
    return hi, (x - hi.astype(F32)).astype(BF16)


def split3(x):
    hi = x.astype(BF16)
    rest = x - hi.astype(F32)
    mid = rest.astype(BF16)
    return hi, mid, (rest - mid.astype(F32)).astype(BF16)


def dot_t(left, right):
    return lax.dot_general(left, right, (((1,), (1,)), ((), ())), preferred_element_type=F32)


def times_t(x, w):
    hi, mid, low = split3(x)
    return dot_t(jnp.concatenate([hi, mid], axis=1), jnp.concatenate([w, w], axis=1)) + dot_t(low, w)


def product(x, w):
    xh, xl = split2(x)
    wh, wl = split2(w)
    return jnp.dot(
        jnp.concatenate([xh, xl, xh], axis=1),
        jnp.concatenate([wh, wh, wl], axis=0),
        preferred_element_type=F32,
    )


PHI, V_ROW, W_MAT, W_ROW, PSI = 0, N, ROWS, ROWS + N, 2 * ROWS
AHEAD, BEHIND = (0, ROWS), (ROWS, MAP - ROWS)


def compose_ahead(left, right, out):
    both = product(left[pl.ds(0, ROWS)], right[pl.ds(PHI, N)])
    out[pl.ds(0, N)] = both[:N]
    out[pl.ds(V_ROW, TR)] = both[N:] + right[pl.ds(V_ROW, TR)]


def compose_behind(left, right, out):
    both = product(left[pl.ds(0, ROWS)], right[pl.ds(W_MAT, N)])
    last = both[N:] + right[pl.ds(W_ROW, TR)]
    back = product(jnp.concatenate([both[:N], last, right[pl.ds(PSI, N)]], axis=0), left[pl.ds(PSI, N)])
    out[pl.ds(W_MAT, ROWS)] = back[:ROWS] + left[pl.ds(W_MAT, ROWS)]
    out[pl.ds(PSI, N)] = back[ROWS:]


def middle_x(x, left):
    return product(x, left[pl.ds(PHI, N)]) + left[pl.ds(V_ROW, TR)]


def tree_of(leaves, nodes):
    levels, used = [leaves], 0
    while len(levels[-1]) > 1:
        row = [nodes.at[used + i] for i in range(len(levels[-1]) // 2)]
        used += len(row)
        levels.append(row)
    return levels


def fill(levels, compose):
    for below, row in zip(levels, levels[1:]):
        for i, node in enumerate(row):
            compose(below[2 * i], below[2 * i + 1], node)


def cross(x_mid, right):
    return product(x_mid, right[pl.ds(W_MAT, N)]) + right[pl.ds(W_ROW, TR)]


def descend_x(x, levels, position):
    plan = []
    for level in range(len(levels) - 2, -1, -1):
        row = levels[level]
        bit = lax.rem(lax.div(position, 2**level), 2)
        above = lax.div(position, 2 ** (level + 1))
        best, terms = None, []
        for i in range(len(row) // 2):
            x_mid = middle_x(x, row[2 * i])
            terms.append((row[2 * i + 1], cross(x_mid, row[2 * i + 1])))
            best = x_mid if best is None else jnp.where(above == i, x_mid, best)
        plan.append((bit, above, terms))
        x = jnp.where(bit == 1, best, x)
    return x, plan


def descend_u(u, plan):
    for bit, above, terms in plan:
        best = None
        for i, (right, term) in enumerate(terms):
            u_mid = product(u, right[pl.ds(PSI, N)]) + term
            best = u_mid if best is None else jnp.where(above == i, u_mid, best)
        u = jnp.where(bit == 1, u, best)
    return u


class Wires:
    def __init__(self, send, recv):
        self.send, self.recv, self.used = send, recv, 0
        self.pending = []

    def make(self, src, dst, **peer):
        copy = pltpu.make_async_remote_copy(
            src_ref=src,
            dst_ref=dst,
            send_sem=self.send.at[self.used],
            recv_sem=self.recv.at[self.used],
            device_id=peer,
            device_id_type=MESH,
        )
        self.used += 1
        return copy

    def go(self, src, dst, **peer):
        copy = self.make(src, dst, **peer)
        copy.start()
        self.pending.append(copy)
        return copy

    def close(self):
        for copy in self.pending:
            copy.wait_send()


def compose_psi(left, right, out):
    out[pl.ds(PSI, N)] = product(right[pl.ds(PSI, N)], left[pl.ds(PSI, N)])


class Ring:
    def __init__(self, wires, buf, axis, size, first, count):
        self.wires, self.buf, self.axis, self.size = wires, buf, axis, size
        self.me = lax.axis_index(axis)
        half = -(-count // 16) * 8
        self.rows = [pl.ds(first, count)]
        if size > 2:
            self.rows = [
                pl.ds(pl.multiple_of(first, 8), half),
                pl.ds(pl.multiple_of(first + half, 8), count - half),
            ]

    def send(self, who, part, there):
        piece = self.buf.at[who, self.rows[part]]
        return self.wires.go(piece, piece, **{self.axis: there})

    def start(self):
        if self.size == 2:
            self.rest = [self.send(self.me, 0, 1 - self.me)]
        if self.size > 2:
            self.right = lax.rem(self.me + 1, self.size)
            self.left = lax.rem(self.me + self.size - 1, self.size)
            self.first = [self.send(self.me, 0, self.right), self.send(self.me, 1, self.left)]
            self.rest = [self.send(self.me, 1, self.right), self.send(self.me, 0, self.left)]

    def relay(self):
        if self.size > 2:
            self.first[0].wait_recv()
            self.rest.append(self.send(self.left, 0, self.right))
            self.first[1].wait_recv()
            self.rest.append(self.send(self.right, 1, self.left))

    def finish(self):
        if self.size > 1:
            for copy in self.rest:
                copy.wait_recv()


class Merge:
    def __init__(self, wires, cand, relay, arrived, y):
        self.wires, self.cand, self.relay_buf, self.arrived, self.y = wires, cand, relay, arrived, y
        self.right, self.left, self.far = (lax.rem(y + k, 4) for k in (1, 3, 2))
        self.each = cand.shape[0] // 4
        self.half = self.each // 2

    def part(self, owner, side):
        return pl.ds(owner * self.each + side * self.half, self.half)

    def start(self):
        go, cand, half = self.wires.go, self.cand, self.half
        low, high = pl.ds(0, half), pl.ds(half, half)
        self.via = [
            go(cand.at[self.part(self.far, 0)], self.relay_buf.at[0], track=self.right),
            go(cand.at[self.part(self.far, 1)], self.relay_buf.at[1], track=self.left),
        ]
        self.rest = [
            go(cand.at[self.part(self.right, 1)], self.arrived.at[0, high], track=self.right),
            go(cand.at[self.part(self.left, 0)], self.arrived.at[1, low], track=self.left),
        ]

    def relay(self):
        go, half = self.wires.go, self.half
        for side, (there, rows) in enumerate(((self.right, pl.ds(0, half)), (self.left, pl.ds(half, half)))):
            self.via[side].wait_recv()
            self.relay_buf[2 + side] = self.relay_buf[side] + self.cand[self.part(there, side)]
            self.rest.append(go(self.relay_buf.at[2 + side], self.arrived.at[side, rows], track=there))

    def finish(self, out):
        for copy in self.rest:
            copy.wait_recv()
        out[...] = self.cand[pl.ds(self.y * self.each, self.each)] + (self.arrived[0] + self.arrived[1])


def forward_pass(a_own, k_own, o_all, x_all, e_all):
    count = a_own.shape[0]
    dwell = o_all.shape[0] // count
    per = count // SEGS
    eye = (
        lax.broadcasted_iota(jnp.int32, (N, N), 0) == lax.broadcasted_iota(jnp.int32, (N, N), 1)
    ).astype(F32)
    start = jnp.concatenate([eye, jnp.zeros((TR, N), F32)], axis=0)
    blank = jnp.zeros((N, N), F32)

    def some(i, xs):
        new_x = list(xs)
        for step in range(dwell):
            for seg in range(SEGS):
                block = seg * per + i
                t = block * dwell + step
                pred = times_t(new_x[seg], a_own[block])
                obs = jnp.concatenate([blank, o_all[t]], axis=0)
                e = k_own[pl.ds(block, 1)] * (obs - pred)
                e_all[t] = e
                x_all[t] = pred + e
                new_x[seg] = pred + e
        return tuple(new_x)

    return lax.fori_loop(0, per, some, (start,) * SEGS)


def backward_pass(g_own, x_all, e_all, hi_ref, lo_ref, s_all, between):
    count = g_own.shape[0]
    dwell = x_all.shape[0] // count
    per = count // SEGS
    eye = (
        lax.broadcasted_iota(jnp.int32, (N, N), 0) == lax.broadcasted_iota(jnp.int32, (N, N), 1)
    ).astype(F32)

    def keep(t, row, value):
        hi, low = split2(value)
        hi_ref[t, pl.ds(row, N)] = hi
        lo_ref[t, pl.ds(row, N)] = low

    def some(i, carry):
        new_u, new_p = list(carry[0]), list(carry[1])
        for step in range(dwell):
            for seg in range(SEGS):
                block = seg * per + per - 1 - i
                t = block * dwell + dwell - 1 - step
                s = x_all[t] + new_u[seg]
                keep(t, 0, s[:N])
                keep(t, N, new_p[seg])
                s_all[t] = s[N:]
                back = times_t(jnp.concatenate([new_u[seg] + e_all[t], new_p[seg]], axis=0), g_own[block])
                new_u[seg], new_p[seg] = back[:ROWS], back[ROWS:]
        return tuple(new_u), tuple(new_p)

    carry = lax.fori_loop(0, per // 2, some, ((jnp.zeros((ROWS, N), F32),) * SEGS, (eye,) * SEGS))
    between()
    return lax.fori_loop(per // 2, per, some, carry)


def response(state, hi_ref, lo_ref, t, row):
    hi, low = split2(state)
    first = jnp.dot(jnp.concatenate([hi, low], axis=0), hi_ref[t, pl.ds(row, N)], preferred_element_type=F32)
    return (first[:TR] + first[TR:]) + jnp.dot(hi, lo_ref[t, pl.ds(row, N)], preferred_element_type=F32)


def final_x(x, levels, hi_ref, lo_ref, s_all):
    xs, plan = [x], []
    for row in levels[-2::-1]:
        new, terms = [], []
        for i, x in enumerate(xs):
            x_mid = middle_x(x, row[2 * i])
            new += [x, x_mid]
            terms.append((row[2 * i + 1], cross(x_mid, row[2 * i + 1])))
        xs = new
        plan.append(terms)
    per = s_all.shape[0] // SEGS
    for seg, x in enumerate(xs):
        for t in range(seg * per, seg * per + per):
            s_all[t] = s_all[t] + response(x, hi_ref, lo_ref, t, 0)
    return plan


def final_u(u, plan, hi_ref, lo_ref, s_all, out_buf, sent):
    us = [u]
    for terms in plan:
        new = []
        for u, (right, term) in zip(us, terms):
            new += [product(u, right[pl.ds(PSI, N)]) + term, u]
        us = new
    per = s_all.shape[0] // SEGS
    four = TR // 4
    for seg, u in enumerate(us):
        for pair in range(per // 2):
            first = seg * per + 2 * pair
            outs = [s_all[t] + response(u, hi_ref, lo_ref, t, N) for t in (first, first + 1)]
            for group in range(4):
                rows = slice(four * group, four * group + four)
                out_buf[group, pl.ds(first * four, 2 * four)] = jnp.concatenate(
                    [outs[0][rows], outs[1][rows]], axis=0
                )
        sent(seg * per * four, per * four)


def main_kernel(sizes, *refs):
    (ids, dyn, smooth, gain, obs_in, out_ref, tab_a, tab_g, tab_s, tab_k, ca, cg, ck, local, relay, arrived, k_buf, o_buf, o_way, a_own, g_own, k_own, o_all, x_all, e_all,
     hi_ref, lo_ref, s_all, segs, segnode, ybuf, ynode, cbuf, cnode, xbuf, xnode, zpv, zps, zc, out_buf,
     send, recv) = refs
    ny, nz, nx, nc = sizes
    y, z, x, c = (lax.axis_index(a) for a in ("track",) + TM)
    each = obs_in.shape[0] // 4
    blocks = a_own.shape[0]
    own_rows = pl.ds(pl.multiple_of(y * each, each), each)
    fetch_a = pltpu.make_async_copy(dyn, tab_a, local.at[0])
    fetch_g = pltpu.make_async_copy(smooth, tab_g, local.at[1])
    fetch_o = pltpu.make_async_copy(obs_in.at[own_rows], o_buf.at[y], local.at[2])
    fetch_k = pltpu.make_async_copy(gain, tab_s, local.at[3])
    for copy in (fetch_k, fetch_a, fetch_g, fetch_o):
        copy.start()
    barrier = pltpu.get_barrier_semaphore()
    peers = []
    for axis, me, size in (("track", y, ny), ("tm_0", z, nz), ("tm_1", x, nx), ("tm_2", c, nc)):
        for step in range(1, size):
            peers.append({axis: lax.rem(me + step, size)})
    for peer in peers:
        pl.semaphore_signal(barrier, inc=1, device_id=peer, device_id_type=MESH)
    fetch_k.wait()
    tab_k[...] = tab_s[...].astype(F32)
    owned = tab_a.shape[0]
    zero_mat = jnp.zeros((N, N), BF16)

    def picked(b):
        row = ids[b] - y * owned
        return jnp.logical_and(row >= 0, row < owned), jnp.clip(row, 0, owned - 1)

    def pick_a(b, _):
        here, row = picked(b)
        ca[b] = jnp.where(here, tab_a[row], zero_mat)
        ck[pl.ds(b, 1)] = jnp.where(here, tab_k[pl.ds(row, 1)], 0.0)
        return 0

    def pick_g(b, _):
        here, row = picked(b)
        cg[b] = jnp.where(here, tab_g[row], zero_mat)
        return 0

    fetch_a.wait()
    lax.fori_loop(0, ca.shape[0], pick_a, 0)
    pl.semaphore_wait(barrier, len(peers))
    wires = Wires(send, recv)
    right, left, far = others = [lax.rem(y + k, 4) for k in (1, 3, 2)]

    a_move = Merge(wires, ca, relay.at[0], arrived.at[0], y)
    g_move = Merge(wires, cg, relay.at[1], arrived.at[1], y)
    a_move.start()
    small = []
    half = each // 2

    def obs_rows(owner, first, count):
        return obs_in.at[pl.ds(pl.multiple_of(owner * each + first, 8), count)]

    for there in (right, left):
        small.append(wires.go(obs_rows(there, 0, each), o_buf.at[y], track=there))
    small.append(wires.go(obs_rows(far, 0, half), o_buf.at[y, pl.ds(0, half)], track=far))
    detour = wires.go(obs_rows(far, half, half), o_way.at[0], track=left)
    for there in others:
        small.append(wires.go(ck.at[pl.ds(pl.multiple_of(there * blocks, blocks), blocks)], k_buf.at[y], track=there))
    k_buf[y] = ck[pl.ds(pl.multiple_of(y * blocks, blocks), blocks)]
    fetch_g.wait()
    lax.fori_loop(0, cg.shape[0], pick_g, 0)
    a_move.relay()
    detour.wait_recv()
    small.append(wires.go(o_way.at[0], o_buf.at[right, pl.ds(half, half)], track=left))
    g_move.start()
    a_move.finish(a_own)
    for copy in small:
        copy.wait_recv()
    fetch_o.wait()
    k_own[...] = (k_buf[0] + k_buf[1]) + (k_buf[2] + k_buf[3])
    four = TR // 4

    def in_steps(p, _):
        tiles = [o_buf[s, pl.ds(pl.multiple_of(p * 2 * four, 8), 2 * four)] for s in range(4)]
        o_all[2 * p] = jnp.concatenate([tile[:four] for tile in tiles], axis=0)
        o_all[2 * p + 1] = jnp.concatenate([tile[four:] for tile in tiles], axis=0)
        return 0

    lax.fori_loop(0, each // (2 * four), in_steps, 0)

    xs = forward_pass(a_own, k_own, o_all, x_all, e_all)
    for seg in range(SEGS):
        segs[seg, pl.ds(0, ROWS)] = xs[seg]
    stree = tree_of([segs.at[i] for i in range(SEGS)], segnode)
    ytree = tree_of([ybuf.at[i] for i in range(ny)], ynode)
    ctree = tree_of([cbuf.at[i] for i in range(nc)], cnode)
    xtree = tree_of([xbuf.at[i] for i in range(nx)], xnode)
    share_a, share_b = AHEAD[1] // nc, BEHIND[1] // nc
    own_a, own_b = c * share_a, BEHIND[0] + c * share_b
    y_ahead = Ring(wires, ybuf, "track", ny, *AHEAD)
    y_behind = Ring(wires, ybuf, "track", ny, *BEHIND)
    c_ahead = Ring(wires, cbuf, "tm_2", nc, *AHEAD)
    c_behind = Ring(wires, cbuf, "tm_2", nc, *BEHIND)
    x_ahead = Ring(wires, xbuf, "tm_1", nx, own_a, share_a)
    x_behind = Ring(wires, xbuf, "tm_1", nx, own_b, share_b)
    fill(stree, compose_ahead)
    ybuf[y, pl.ds(0, ROWS)] = stree[-1][0][pl.ds(0, ROWS)]
    g_move.relay()
    y_ahead.start()
    g_move.finish(g_own)

    us, ps = backward_pass(g_own, x_all, e_all, hi_ref, lo_ref, s_all, y_ahead.relay)
    for seg in range(SEGS):
        segs[seg, pl.ds(W_MAT, ROWS)] = us[seg]
        segs[seg, pl.ds(PSI, N)] = ps[seg]
    fill(stree, compose_behind)
    ybuf[y, pl.ds(W_MAT, ROWS + N)] = stree[-1][0][pl.ds(W_MAT, ROWS + N)]
    y_behind.start()

    def share_start(own, share):
        rows = pl.ds(pl.multiple_of(own, 8), share)
        parts = [xbuf.at[lax.rem(x + step, nx), rows] for step in range(1, nx)] if nc > 1 else []
        return [wires.go(part, part, tm_2=1 - c) for part in parts]

    far_first = sorted(range(1, nz), key=lambda step: -min(step, nz - step))

    def to_slabs(buf, rows, later):
        mine = pl.ds(pl.multiple_of(c * (rows // nc), 8), rows // nc)
        part = buf.at[z, mine]
        moves = {}
        for step in far_first:
            there = z + step if later else z - step
            copy = wires.make(part, part, tm_0=jnp.clip(there, 0, nz - 1))
            use = there < nz if later else jnp.logical_and(there >= 0, z < nz - 1)
            moves[step] = (copy, use)
            pl.when(use)(copy.start)
        return mine, moves

    def from_slabs(buf, mine, moves, later):
        shared = []
        for step in far_first[::-1]:
            copy = moves[step][0]
            source = z - step if later else z + step
            use = source >= 0 if later else source < nz - 1
            pl.when(use)(copy.wait_recv)
            if nc > 1:
                part = buf.at[jnp.clip(source, 0, nz - 1), mine]
                over = wires.make(part, part, tm_2=1 - c)
                pl.when(use)(over.start)
                shared.append((over, use))
        for copy, use in shared:
            pl.when(use)(copy.wait_recv)
        for copy, use in list(moves.values()) + shared:
            pl.when(use)(copy.wait_send)

    y_ahead.finish()
    fill(ytree, compose_ahead)
    cbuf[c, pl.ds(0, ROWS)] = ytree[-1][0][pl.ds(0, ROWS)]
    c_ahead.start()
    c_ahead.finish()
    fill(ctree, compose_ahead)
    xbuf[x, pl.ds(0, ROWS)] = ctree[-1][0][pl.ds(0, ROWS)]
    x_ahead.start()
    y_behind.relay()
    x_ahead.relay()
    y_behind.finish()
    x_ahead.finish()
    shared = share_start(own_a, share_a)
    fill(ytree, compose_behind)
    cbuf[c, pl.ds(W_MAT, ROWS + N)] = ytree[-1][0][pl.ds(W_MAT, ROWS + N)]
    c_behind.start()
    for copy in shared:
        copy.wait_recv()
    fill(xtree, compose_ahead)
    total = xtree[-1][0]
    zpv[z] = total[pl.ds(0, ROWS)]
    z_ahead = to_slabs(zpv, ROWS, True)
    c_behind.finish()
    fill(ctree, compose_behind)
    xbuf[x, pl.ds(W_MAT, ROWS + N)] = ctree[-1][0][pl.ds(W_MAT, ROWS + N)]
    x_behind.start()
    x_behind.relay()
    from_slabs(zpv, *z_ahead, True)

    zero = jnp.zeros((TR, N), F32)
    entering, state = zero, zero
    for i in range(nz - 1):
        got = jnp.minimum(i, z)
        after = zpv[got, pl.ds(V_ROW, TR)]
        if i > 0:
            after = after + product(state, zpv[got, pl.ds(PHI, N)])
        state = after
        entering = jnp.where(z == i + 1, state, entering)
    chip_x = [entering]
    for i in range(nx - 1):
        chip_x.append(middle_x(chip_x[-1], xbuf.at[i]))
    x_behind.finish()
    for copy in share_start(own_b, share_b):
        copy.wait_recv()
    fill(xtree, compose_psi)
    zps[z] = total[pl.ds(PSI, N)]
    z_behind = to_slabs(zps, N, False)
    chip_w = [product(chip_x[i], xbuf[i, pl.ds(W_MAT, N)]) + xbuf[i, pl.ds(W_ROW, TR)] for i in range(nx)]

    def leave_chips(state):
        states = [state]
        for i in range(nx - 1, -1, -1):
            states.append(chip_w[i] if states[-1] is None else product(states[-1], xbuf[i, pl.ds(PSI, N)]) + chip_w[i])
        return states[::-1]

    zc[z] = leave_chips(None)[0]
    part = zc.at[z]
    group = [wires.go(part, part, tm_0=lax.rem(z + step, nz)) for step in far_first]
    xv = chip_x[0]
    for i in range(1, nx):
        xv = jnp.where(x == i, chip_x[i], xv)
    xv, c_plan = descend_x(xv, ctree, c)
    xv, y_plan = descend_x(xv, ytree, y)
    s_plan = final_x(xv, stree, hi_ref, lo_ref, s_all)
    from_slabs(zps, *z_behind, False)
    for copy in group:
        copy.wait_recv()
    leaving, state = zero, zero
    for i in range(nz - 1, 0, -1):
        after = zc[i]
        if i < nz - 1:
            after = after + product(state, zps[jnp.maximum(i, z)])
        state = after
        leaving = jnp.where(z == i - 1, state, leaving)

    chip_u = leave_chips(leaving)
    uv = chip_u[1]
    for i in range(1, nx):
        uv = jnp.where(x == i, chip_u[i + 1], uv)
    uv = descend_u(descend_u(uv, c_plan), y_plan)

    homes, detours = [], []

    def target(first, count):
        return out_ref.at[pl.ds(pl.multiple_of(y * each + first, 8), count)]

    def sent(first, count):
        rows = pl.ds(first, count)
        if first < half:
            detours.append((wires.go(out_buf.at[far, rows], o_way.at[1, rows], track=left), rows, first, count))
        for there in (right, left) if first < half else others:
            homes.append(wires.go(out_buf.at[there, rows], target(first, count), track=there))

    final_u(uv, s_plan, hi_ref, lo_ref, s_all, out_buf, sent)
    out_ref[own_rows] = out_buf[y]
    for copy, rows, first, count in detours:
        copy.wait_recv()
        there = out_ref.at[pl.ds(pl.multiple_of(right * each + first, 8), count)]
        homes.append(wires.go(o_way.at[1, rows], there, track=left))
    for copy in homes:
        copy.wait_recv()
    wires.close()


def main_call(sizes, ids, dyn, smooth, gain, obs):
    ny, nz, nx, nc = sizes
    count, owned = ids.shape[0], dyn.shape[0]
    blocks = count // ny
    each = obs.shape[0] // ny
    steps = each // (TR // ny)
    links = 20 + 30 + 2 * (1 + nx) + 5 * nz + 3 * SEGS
    hbm = pl.BlockSpec(memory_space=pltpu.MemorySpace.HBM)
    vmem = pl.BlockSpec(memory_space=VMEM)
    return pl.pallas_call(
        functools.partial(main_kernel, sizes),
        out_shape=jax.ShapeDtypeStruct(obs.shape, F32),
        in_specs=[pl.BlockSpec(memory_space=pltpu.MemorySpace.SMEM), hbm, hbm, hbm, hbm],
        out_specs=vmem,
        scratch_shapes=[
            pltpu.VMEM((owned, N, N), BF16),
            pltpu.VMEM((owned, N, N), BF16),
            pltpu.VMEM((owned, N), BF16),
            pltpu.VMEM((owned, N), F32),
            pltpu.VMEM((count, N, N), BF16),
            pltpu.VMEM((count, N, N), BF16),
            pltpu.VMEM((count, N), F32),
            pltpu.SemaphoreType.DMA((4,)),
            pltpu.VMEM((2, 4, blocks // 2, N, N), BF16),
            pltpu.VMEM((2, 2, blocks, N, N), BF16),
            pltpu.VMEM((4, blocks, N), F32),
            pltpu.VMEM((4, each, N), F32),
            pltpu.VMEM((2, each // 2, N), F32),
            pltpu.VMEM((blocks, N, N), BF16),
            pltpu.VMEM((blocks, N, N), BF16),
            pltpu.VMEM((blocks, N), F32),
            pltpu.VMEM((steps, TR, N), F32),
            pltpu.VMEM((steps, ROWS, N), F32),
            pltpu.VMEM((steps, ROWS, N), F32),
            pltpu.VMEM((steps, 2 * N, N), BF16),
            pltpu.VMEM((steps, 2 * N, N), BF16),
            pltpu.VMEM((steps, TR, N), F32),
            pltpu.VMEM((SEGS, MAP, N), F32),
            pltpu.VMEM((SEGS - 1, MAP, N), F32),
            pltpu.VMEM((ny, MAP, N), F32),
            pltpu.VMEM((max(ny - 1, 1), MAP, N), F32),
            pltpu.VMEM((nc, MAP, N), F32),
            pltpu.VMEM((max(nc - 1, 1), MAP, N), F32),
            pltpu.VMEM((nx, MAP, N), F32),
            pltpu.VMEM((max(nx - 1, 1), MAP, N), F32),
            pltpu.VMEM((nz, ROWS, N), F32),
            pltpu.VMEM((nz, N, N), F32),
            pltpu.VMEM((nz, TR, N), F32),
            pltpu.VMEM((4, each, N), F32),
            pltpu.SemaphoreType.DMA((links,)),
            pltpu.SemaphoreType.DMA((links,)),
        ],
        compiler_params=pltpu.CompilerParams(
            collective_id=1, has_side_effects=True, vmem_limit_bytes=67043328
        ),
        name="smooth",
    )(ids, dyn, smooth, gain, obs)


def body(sizes, observations, dynamics, smoother_gain, gains, regime):
    out = main_call(sizes, regime, dynamics, smoother_gain, gains, observations.reshape(-1, N))
    return out.reshape(observations.shape)


def build(torus):
    sizes = tuple(torus.shape[a] for a in ("track",) + TM)
    placed = (
        P(TM, "track", None),
        P("track", None, None),
        P("track", None, None),
        P("track", None),
        P(TM),
    )
    return jax.shard_map(
        functools.partial(body, sizes),
        mesh=torus,
        in_specs=placed,
        out_specs=P(TM, "track", None),
        check_vma=False,
    )


def solution(mesh):
    return build(Mesh(mesh.devices.reshape(mesh.shape["track"], 8, 4, 2), ("track",) + TM))
```

```python
import functools

import jax
import jax.numpy as jnp
import numpy as np
from jax import lax
from jax.experimental import pallas as pl
from jax.experimental.pallas import tpu as pltpu
from jax.sharding import Mesh
from jax.sharding import PartitionSpec as P

TM = ("tm_0", "tm_1", "tm_2")
F32 = jnp.float32
BF16 = jnp.bfloat16
N = 128
TR = 16
ROWS = N + TR
MAP = 2 * ROWS + N
SEGS = 4
MESH = pl.DeviceIdType.MESH
VMEM = pltpu.MemorySpace.VMEM


def split2(x):
    hi = x.astype(BF16)
    return hi, (x - hi.astype(F32)).astype(BF16)


def split3(x):
    hi = x.astype(BF16)
    rest = x - hi.astype(F32)
    mid = rest.astype(BF16)
    return hi, mid, (rest - mid.astype(F32)).astype(BF16)


def dot_t(left, right):
    return lax.dot_general(left, right, (((1,), (1,)), ((), ())), preferred_element_type=F32)


def times_t(x, w):
    hi, mid, low = split3(x)
    return dot_t(jnp.concatenate([hi, mid], axis=1), jnp.concatenate([w, w], axis=1)) + dot_t(low, w)


def product(x, w):
    xh, xl = split2(x)
    wh, wl = split2(w)
    return jnp.dot(
        jnp.concatenate([xh, xl, xh], axis=1),
        jnp.concatenate([wh, wh, wl], axis=0),
        preferred_element_type=F32,
    )


PHI, V_ROW, W_MAT, W_ROW, PSI = 0, N, ROWS, ROWS + N, 2 * ROWS
AHEAD, BEHIND = (0, ROWS), (ROWS, MAP - ROWS)


def compose_ahead(left, right, out):
    both = product(left[pl.ds(0, ROWS)], right[pl.ds(PHI, N)])
    out[pl.ds(0, N)] = both[:N]
    out[pl.ds(V_ROW, TR)] = both[N:] + right[pl.ds(V_ROW, TR)]


def compose_behind(left, right, out):
    both = product(left[pl.ds(0, ROWS)], right[pl.ds(W_MAT, N)])
    last = both[N:] + right[pl.ds(W_ROW, TR)]
    back = product(jnp.concatenate([both[:N], last, right[pl.ds(PSI, N)]], axis=0), left[pl.ds(PSI, N)])
    out[pl.ds(W_MAT, ROWS)] = back[:ROWS] + left[pl.ds(W_MAT, ROWS)]
    out[pl.ds(PSI, N)] = back[ROWS:]


def middle_x(x, left):
    return product(x, left[pl.ds(PHI, N)]) + left[pl.ds(V_ROW, TR)]


def tree_of(leaves, nodes):
    levels, used = [leaves], 0
    while len(levels[-1]) > 1:
        row = [nodes.at[used + i] for i in range(len(levels[-1]) // 2)]
        used += len(row)
        levels.append(row)
    return levels


def fill(levels, compose):
    for below, row in zip(levels, levels[1:]):
        for i, node in enumerate(row):
            compose(below[2 * i], below[2 * i + 1], node)


def cross(x_mid, right):
    return product(x_mid, right[pl.ds(W_MAT, N)]) + right[pl.ds(W_ROW, TR)]


def descend_x(x, levels, position):
    plan = []
    for level in range(len(levels) - 2, -1, -1):
        row = levels[level]
        bit = lax.rem(lax.div(position, 2**level), 2)
        above = lax.div(position, 2 ** (level + 1))
        best, terms = None, []
        for i in range(len(row) // 2):
            x_mid = middle_x(x, row[2 * i])
            terms.append((row[2 * i + 1], cross(x_mid, row[2 * i + 1])))
            best = x_mid if best is None else jnp.where(above == i, x_mid, best)
        plan.append((bit, above, terms))
        x = jnp.where(bit == 1, best, x)
    return x, plan


def descend_u(u, plan):
    for bit, above, terms in plan:
        best = None
        for i, (right, term) in enumerate(terms):
            u_mid = product(u, right[pl.ds(PSI, N)]) + term
            best = u_mid if best is None else jnp.where(above == i, u_mid, best)
        u = jnp.where(bit == 1, u, best)
    return u


class Wires:
    def __init__(self, send, recv):
        self.send, self.recv, self.used = send, recv, 0
        self.pending = []

    def make(self, src, dst, **peer):
        copy = pltpu.make_async_remote_copy(
            src_ref=src,
            dst_ref=dst,
            send_sem=self.send.at[self.used],
            recv_sem=self.recv.at[self.used],
            device_id=peer,
            device_id_type=MESH,
        )
        self.used += 1
        return copy

    def go(self, src, dst, **peer):
        copy = self.make(src, dst, **peer)
        copy.start()
        self.pending.append(copy)
        return copy

    def close(self):
        for copy in self.pending:
            copy.wait_send()


def compose_psi(left, right, out):
    out[pl.ds(PSI, N)] = product(right[pl.ds(PSI, N)], left[pl.ds(PSI, N)])


class Ring:
    def __init__(self, wires, buf, axis, size, first, count):
        self.wires, self.buf, self.axis, self.size = wires, buf, axis, size
        self.me = lax.axis_index(axis)
        half = -(-count // 16) * 8
        self.rows = [pl.ds(first, count)]
        if size > 2:
            self.rows = [
                pl.ds(pl.multiple_of(first, 8), half),
                pl.ds(pl.multiple_of(first + half, 8), count - half),
            ]

    def send(self, who, part, there):
        piece = self.buf.at[who, self.rows[part]]
        return self.wires.go(piece, piece, **{self.axis: there})

    def start(self):
        if self.size == 2:
            self.rest = [self.send(self.me, 0, 1 - self.me)]
        if self.size > 2:
            self.right = lax.rem(self.me + 1, self.size)
            self.left = lax.rem(self.me + self.size - 1, self.size)
            self.first = [self.send(self.me, 0, self.right), self.send(self.me, 1, self.left)]
            self.rest = [self.send(self.me, 1, self.right), self.send(self.me, 0, self.left)]

    def relay(self):
        if self.size > 2:
            self.first[0].wait_recv()
            self.rest.append(self.send(self.left, 0, self.right))
            self.first[1].wait_recv()
            self.rest.append(self.send(self.right, 1, self.left))

    def finish(self):
        if self.size > 1:
            for copy in self.rest:
                copy.wait_recv()


class Merge:
    def __init__(self, wires, cand, relay, arrived, y):
        self.wires, self.cand, self.relay_buf, self.arrived, self.y = wires, cand, relay, arrived, y
        self.right, self.left, self.far = (lax.rem(y + k, 4) for k in (1, 3, 2))
        self.each = cand.shape[0] // 4
        self.half = self.each // 2

    def part(self, owner, side):
        return pl.ds(owner * self.each + side * self.half, self.half)

    def start(self):
        go, cand, half = self.wires.go, self.cand, self.half
        low, high = pl.ds(0, half), pl.ds(half, half)
        self.via = [
            go(cand.at[self.part(self.far, 0)], self.relay_buf.at[0], track=self.right),
            go(cand.at[self.part(self.far, 1)], self.relay_buf.at[1], track=self.left),
        ]
        self.rest = [
            go(cand.at[self.part(self.right, 1)], self.arrived.at[0, high], track=self.right),
            go(cand.at[self.part(self.left, 0)], self.arrived.at[1, low], track=self.left),
        ]

    def relay(self):
        go, half = self.wires.go, self.half
        for side, (there, rows) in enumerate(((self.right, pl.ds(0, half)), (self.left, pl.ds(half, half)))):
            self.via[side].wait_recv()
            self.relay_buf[2 + side] = self.relay_buf[side] + self.cand[self.part(there, side)]
            self.rest.append(go(self.relay_buf.at[2 + side], self.arrived.at[side, rows], track=there))

    def finish(self, out):
        for copy in self.rest:
            copy.wait_recv()
        out[...] = self.cand[pl.ds(self.y * self.each, self.each)] + (self.arrived[0] + self.arrived[1])


def forward_pass(a_own, k_own, o_all, x_all, e_all):
    count = a_own.shape[0]
    dwell = o_all.shape[0] // count
    per = count // SEGS
    eye = (
        lax.broadcasted_iota(jnp.int32, (N, N), 0) == lax.broadcasted_iota(jnp.int32, (N, N), 1)
    ).astype(F32)
    start = jnp.concatenate([eye, jnp.zeros((TR, N), F32)], axis=0)
    blank = jnp.zeros((N, N), F32)

    def some(i, xs):
        new_x = list(xs)
        for step in range(dwell):
            for seg in range(SEGS):
                block = seg * per + i
                t = block * dwell + step
                pred = times_t(new_x[seg], a_own[block])
                obs = jnp.concatenate([blank, o_all[t]], axis=0)
                e = k_own[pl.ds(block, 1)] * (obs - pred)
                e_all[t] = e
                x_all[t] = pred + e
                new_x[seg] = pred + e
        return tuple(new_x)

    return lax.fori_loop(0, per, some, (start,) * SEGS)


def backward_pass(g_own, x_all, e_all, hi_ref, lo_ref, s_all, between):
    count = g_own.shape[0]
    dwell = x_all.shape[0] // count
    per = count // SEGS
    eye = (
        lax.broadcasted_iota(jnp.int32, (N, N), 0) == lax.broadcasted_iota(jnp.int32, (N, N), 1)
    ).astype(F32)

    def keep(t, row, value):
        hi, low = split2(value)
        hi_ref[t, pl.ds(row, N)] = hi
        lo_ref[t, pl.ds(row, N)] = low

    def some(i, carry):
        new_u, new_p = list(carry[0]), list(carry[1])
        for step in range(dwell):
            for seg in range(SEGS):
                block = seg * per + per - 1 - i
                t = block * dwell + dwell - 1 - step
                s = x_all[t] + new_u[seg]
                keep(t, 0, s[:N])
                keep(t, N, new_p[seg])
                s_all[t] = s[N:]
                back = times_t(jnp.concatenate([new_u[seg] + e_all[t], new_p[seg]], axis=0), g_own[block])
                new_u[seg], new_p[seg] = back[:ROWS], back[ROWS:]
        return tuple(new_u), tuple(new_p)

    carry = lax.fori_loop(0, per // 2, some, ((jnp.zeros((ROWS, N), F32),) * SEGS, (eye,) * SEGS))
    between()
    return lax.fori_loop(per // 2, per, some, carry)


def response(state, hi_ref, lo_ref, t, row):
    hi, low = split2(state)
    first = jnp.dot(jnp.concatenate([hi, low], axis=0), hi_ref[t, pl.ds(row, N)], preferred_element_type=F32)
    return (first[:TR] + first[TR:]) + jnp.dot(hi, lo_ref[t, pl.ds(row, N)], preferred_element_type=F32)


def final_x(x, levels, hi_ref, lo_ref, s_all):
    xs, plan = [x], []
    for row in levels[-2::-1]:
        new, terms = [], []
        for i, x in enumerate(xs):
            x_mid = middle_x(x, row[2 * i])
            new += [x, x_mid]
            terms.append((row[2 * i + 1], cross(x_mid, row[2 * i + 1])))
        xs = new
        plan.append(terms)
    per = s_all.shape[0] // SEGS
    for seg, x in enumerate(xs):
        for t in range(seg * per, seg * per + per):
            s_all[t] = s_all[t] + response(x, hi_ref, lo_ref, t, 0)
    return plan


def final_u(u, plan, hi_ref, lo_ref, s_all, out_buf, sent):
    us = [u]
    for terms in plan:
        new = []
        for u, (right, term) in zip(us, terms):
            new += [product(u, right[pl.ds(PSI, N)]) + term, u]
        us = new
    per = s_all.shape[0] // SEGS
    four = TR // 4
    for seg, u in enumerate(us):
        for pair in range(per // 2):
            first = seg * per + 2 * pair
            outs = [s_all[t] + response(u, hi_ref, lo_ref, t, N) for t in (first, first + 1)]
            for group in range(4):
                rows = slice(four * group, four * group + four)
                out_buf[group, pl.ds(first * four, 2 * four)] = jnp.concatenate(
                    [outs[0][rows], outs[1][rows]], axis=0
                )
        sent(seg * per * four, per * four)


def main_kernel(sizes, *refs):
    (ids, dyn, smooth, gain, obs_in, out_ref, tab_a, tab_g, tab_s, tab_k, ca, cg, ck, local, relay, arrived, k_buf, o_buf, o_way, a_own, g_own, k_own, o_all, x_all, e_all,
     hi_ref, lo_ref, s_all, segs, segnode, ybuf, ynode, cbuf, cnode, xbuf, xnode, zpv, zps, zc, out_buf,
     send, recv) = refs
    ny, nz, nx, nc = sizes
    y, z, x, c = (lax.axis_index(a) for a in ("track",) + TM)
    each = obs_in.shape[0] // 4
    blocks = a_own.shape[0]
    own_rows = pl.ds(pl.multiple_of(y * each, each), each)
    fetch_a = pltpu.make_async_copy(dyn, tab_a, local.at[0])
    fetch_g = pltpu.make_async_copy(smooth, tab_g, local.at[1])
    fetch_o = pltpu.make_async_copy(obs_in.at[own_rows], o_buf.at[y], local.at[2])
    fetch_k = pltpu.make_async_copy(gain, tab_s, local.at[3])
    for copy in (fetch_k, fetch_a, fetch_g, fetch_o):
        copy.start()
    barrier = pltpu.get_barrier_semaphore()
    peers = []
    for axis, me, size in (("track", y, ny), ("tm_0", z, nz), ("tm_1", x, nx), ("tm_2", c, nc)):
        for step in range(1, size):
            peers.append({axis: lax.rem(me + step, size)})
    for peer in peers:
        pl.semaphore_signal(barrier, inc=1, device_id=peer, device_id_type=MESH)
    fetch_k.wait()
    tab_k[...] = tab_s[...].astype(F32)
    owned = tab_a.shape[0]
    zero_mat = jnp.zeros((N, N), BF16)

    def picked(b):
        row = ids[b] - y * owned
        return jnp.logical_and(row >= 0, row < owned), jnp.clip(row, 0, owned - 1)

    def pick_a(b, _):
        here, row = picked(b)
        ca[b] = jnp.where(here, tab_a[row], zero_mat)
        ck[pl.ds(b, 1)] = jnp.where(here, tab_k[pl.ds(row, 1)], 0.0)
        return 0

    def pick_g(b, _):
        here, row = picked(b)
        cg[b] = jnp.where(here, tab_g[row], zero_mat)
        return 0

    fetch_a.wait()
    lax.fori_loop(0, ca.shape[0], pick_a, 0)
    pl.semaphore_wait(barrier, len(peers))
    wires = Wires(send, recv)
    right, left, far = others = [lax.rem(y + k, 4) for k in (1, 3, 2)]

    a_move = Merge(wires, ca, relay.at[0], arrived.at[0], y)
    g_move = Merge(wires, cg, relay.at[1], arrived.at[1], y)
    a_move.start()
    small = []
    half = each // 2

    def obs_rows(owner, first, count):
        return obs_in.at[pl.ds(pl.multiple_of(owner * each + first, 8), count)]

    for there in (right, left):
        small.append(wires.go(obs_rows(there, 0, each), o_buf.at[y], track=there))
    small.append(wires.go(obs_rows(far, 0, half), o_buf.at[y, pl.ds(0, half)], track=far))
    detour = wires.go(obs_rows(far, half, half), o_way.at[0], track=left)
    for there in others:
        small.append(wires.go(ck.at[pl.ds(pl.multiple_of(there * blocks, blocks), blocks)], k_buf.at[y], track=there))
    k_buf[y] = ck[pl.ds(pl.multiple_of(y * blocks, blocks), blocks)]
    fetch_g.wait()
    lax.fori_loop(0, cg.shape[0], pick_g, 0)
    a_move.relay()
    detour.wait_recv()
    small.append(wires.go(o_way.at[0], o_buf.at[right, pl.ds(half, half)], track=left))
    g_move.start()
    a_move.finish(a_own)
    for copy in small:
        copy.wait_recv()
    fetch_o.wait()
    k_own[...] = (k_buf[0] + k_buf[1]) + (k_buf[2] + k_buf[3])
    four = TR // 4

    def in_steps(p, _):
        tiles = [o_buf[s, pl.ds(pl.multiple_of(p * 2 * four, 8), 2 * four)] for s in range(4)]
        o_all[2 * p] = jnp.concatenate([tile[:four] for tile in tiles], axis=0)
        o_all[2 * p + 1] = jnp.concatenate([tile[four:] for tile in tiles], axis=0)
        return 0

    lax.fori_loop(0, each // (2 * four), in_steps, 0)

    xs = forward_pass(a_own, k_own, o_all, x_all, e_all)
    for seg in range(SEGS):
        segs[seg, pl.ds(0, ROWS)] = xs[seg]
    stree = tree_of([segs.at[i] for i in range(SEGS)], segnode)
    ytree = tree_of([ybuf.at[i] for i in range(ny)], ynode)
    ctree = tree_of([cbuf.at[i] for i in range(nc)], cnode)
    xtree = tree_of([xbuf.at[i] for i in range(nx)], xnode)
    share_a, share_b = AHEAD[1] // nc, BEHIND[1] // nc
    own_a, own_b = c * share_a, BEHIND[0] + c * share_b
    y_ahead = Ring(wires, ybuf, "track", ny, *AHEAD)
    y_behind = Ring(wires, ybuf, "track", ny, *BEHIND)
    c_ahead = Ring(wires, cbuf, "tm_2", nc, *AHEAD)
    c_behind = Ring(wires, cbuf, "tm_2", nc, *BEHIND)
    x_ahead = Ring(wires, xbuf, "tm_1", nx, own_a, share_a)
    x_behind = Ring(wires, xbuf, "tm_1", nx, own_b, share_b)
    fill(stree, compose_ahead)
    ybuf[y, pl.ds(0, ROWS)] = stree[-1][0][pl.ds(0, ROWS)]
    g_move.relay()
    y_ahead.start()
    g_move.finish(g_own)

    us, ps = backward_pass(g_own, x_all, e_all, hi_ref, lo_ref, s_all, y_ahead.relay)
    for seg in range(SEGS):
        segs[seg, pl.ds(W_MAT, ROWS)] = us[seg]
        segs[seg, pl.ds(PSI, N)] = ps[seg]
    fill(stree, compose_behind)
    ybuf[y, pl.ds(W_MAT, ROWS + N)] = stree[-1][0][pl.ds(W_MAT, ROWS + N)]
    y_behind.start()

    def share_start(own, share):
        rows = pl.ds(pl.multiple_of(own, 8), share)
        parts = [xbuf.at[lax.rem(x + step, nx), rows] for step in range(1, nx)] if nc > 1 else []
        return [wires.go(part, part, tm_2=1 - c) for part in parts]

    far_first = sorted(range(1, nz), key=lambda step: -min(step, nz - step))

    def to_slabs(buf, rows, later):
        mine = pl.ds(pl.multiple_of(c * (rows // nc), 8), rows // nc)
        part = buf.at[z, mine]
        moves = {}
        for step in far_first:
            there = z + step if later else z - step
            copy = wires.make(part, part, tm_0=jnp.clip(there, 0, nz - 1))
            use = there < nz if later else jnp.logical_and(there >= 0, z < nz - 1)
            moves[step] = (copy, use)
            pl.when(use)(copy.start)
        return mine, moves

    def from_slabs(buf, mine, moves, later):
        shared = []
        for step in far_first[::-1]:
            copy = moves[step][0]
            source = z - step if later else z + step
            use = source >= 0 if later else source < nz - 1
            pl.when(use)(copy.wait_recv)
            if nc > 1:
                part = buf.at[jnp.clip(source, 0, nz - 1), mine]
                over = wires.make(part, part, tm_2=1 - c)
                pl.when(use)(over.start)
                shared.append((over, use))
        for copy, use in shared:
            pl.when(use)(copy.wait_recv)
        for copy, use in list(moves.values()) + shared:
            pl.when(use)(copy.wait_send)

    y_ahead.finish()
    fill(ytree, compose_ahead)
    cbuf[c, pl.ds(0, ROWS)] = ytree[-1][0][pl.ds(0, ROWS)]
    c_ahead.start()
    c_ahead.finish()
    fill(ctree, compose_ahead)
    xbuf[x, pl.ds(0, ROWS)] = ctree[-1][0][pl.ds(0, ROWS)]
    x_ahead.start()
    y_behind.relay()
    x_ahead.relay()
    y_behind.finish()
    fill(ytree, compose_behind)
    cbuf[c, pl.ds(W_MAT, ROWS + N)] = ytree[-1][0][pl.ds(W_MAT, ROWS + N)]
    c_behind.start()
    x_ahead.finish()
    shared = share_start(own_a, share_a)
    c_behind.finish()
    fill(ctree, compose_behind)
    xbuf[x, pl.ds(W_MAT, ROWS + N)] = ctree[-1][0][pl.ds(W_MAT, ROWS + N)]
    x_behind.start()
    for copy in shared:
        copy.wait_recv()
    fill(xtree, compose_ahead)
    total = xtree[-1][0]
    zpv[z] = total[pl.ds(0, ROWS)]
    z_ahead = to_slabs(zpv, ROWS, True)
    x_behind.relay()
    x_behind.finish()
    for copy in share_start(own_b, share_b):
        copy.wait_recv()
    fill(xtree, compose_psi)
    zps[z] = total[pl.ds(PSI, N)]
    z_behind = to_slabs(zps, N, False)
    from_slabs(zpv, *z_ahead, True)

    zero = jnp.zeros((TR, N), F32)
    entering, state = zero, zero
    for i in range(nz - 1):
        got = jnp.minimum(i, z)
        after = zpv[got, pl.ds(V_ROW, TR)]
        if i > 0:
            after = after + product(state, zpv[got, pl.ds(PHI, N)])
        state = after
        entering = jnp.where(z == i + 1, state, entering)
    chip_x = [entering]
    for i in range(nx - 1):
        chip_x.append(middle_x(chip_x[-1], xbuf.at[i]))
    chip_w = [product(chip_x[i], xbuf[i, pl.ds(W_MAT, N)]) + xbuf[i, pl.ds(W_ROW, TR)] for i in range(nx)]

    def leave_chips(state):
        states = [state]
        for i in range(nx - 1, -1, -1):
            states.append(chip_w[i] if states[-1] is None else product(states[-1], xbuf[i, pl.ds(PSI, N)]) + chip_w[i])
        return states[::-1]

    zc[z] = leave_chips(None)[0]
    part = zc.at[z]
    group = [wires.go(part, part, tm_0=lax.rem(z + step, nz)) for step in far_first]
    xv = chip_x[0]
    for i in range(1, nx):
        xv = jnp.where(x == i, chip_x[i], xv)
    xv, c_plan = descend_x(xv, ctree, c)
    xv, y_plan = descend_x(xv, ytree, y)
    s_plan = final_x(xv, stree, hi_ref, lo_ref, s_all)
    from_slabs(zps, *z_behind, False)
    for copy in group:
        copy.wait_recv()
    leaving, state = zero, zero
    for i in range(nz - 1, 0, -1):
        after = zc[i]
        if i < nz - 1:
            after = after + product(state, zps[jnp.maximum(i, z)])
        state = after
        leaving = jnp.where(z == i - 1, state, leaving)

    chip_u = leave_chips(leaving)
    uv = chip_u[1]
    for i in range(1, nx):
        uv = jnp.where(x == i, chip_u[i + 1], uv)
    uv = descend_u(descend_u(uv, c_plan), y_plan)

    homes, detours = [], []

    def target(first, count):
        return out_ref.at[pl.ds(pl.multiple_of(y * each + first, 8), count)]

    def sent(first, count):
        rows = pl.ds(first, count)
        if first < half:
            detours.append((wires.go(out_buf.at[far, rows], o_way.at[1, rows], track=left), rows, first, count))
        for there in (right, left) if first < half else others:
            homes.append(wires.go(out_buf.at[there, rows], target(first, count), track=there))

    final_u(uv, s_plan, hi_ref, lo_ref, s_all, out_buf, sent)
    out_ref[own_rows] = out_buf[y]
    for copy, rows, first, count in detours:
        copy.wait_recv()
        there = out_ref.at[pl.ds(pl.multiple_of(right * each + first, 8), count)]
        homes.append(wires.go(o_way.at[1, rows], there, track=left))
    for copy in homes:
        copy.wait_recv()
    wires.close()


def main_call(sizes, ids, dyn, smooth, gain, obs):
    ny, nz, nx, nc = sizes
    count, owned = ids.shape[0], dyn.shape[0]
    blocks = count // ny
    each = obs.shape[0] // ny
    steps = each // (TR // ny)
    links = 20 + 30 + 2 * (1 + nx) + 5 * nz + 3 * SEGS
    hbm = pl.BlockSpec(memory_space=pltpu.MemorySpace.HBM)
    vmem = pl.BlockSpec(memory_space=VMEM)
    return pl.pallas_call(
        functools.partial(main_kernel, sizes),
        out_shape=jax.ShapeDtypeStruct(obs.shape, F32),
        in_specs=[pl.BlockSpec(memory_space=pltpu.MemorySpace.SMEM), hbm, hbm, hbm, hbm],
        out_specs=vmem,
        scratch_shapes=[
            pltpu.VMEM((owned, N, N), BF16),
            pltpu.VMEM((owned, N, N), BF16),
            pltpu.VMEM((owned, N), BF16),
            pltpu.VMEM((owned, N), F32),
            pltpu.VMEM((count, N, N), BF16),
            pltpu.VMEM((count, N, N), BF16),
            pltpu.VMEM((count, N), F32),
            pltpu.SemaphoreType.DMA((4,)),
            pltpu.VMEM((2, 4, blocks // 2, N, N), BF16),
            pltpu.VMEM((2, 2, blocks, N, N), BF16),
            pltpu.VMEM((4, blocks, N), F32),
            pltpu.VMEM((4, each, N), F32),
            pltpu.VMEM((2, each // 2, N), F32),
            pltpu.VMEM((blocks, N, N), BF16),
            pltpu.VMEM((blocks, N, N), BF16),
            pltpu.VMEM((blocks, N), F32),
            pltpu.VMEM((steps, TR, N), F32),
            pltpu.VMEM((steps, ROWS, N), F32),
            pltpu.VMEM((steps, ROWS, N), F32),
            pltpu.VMEM((steps, 2 * N, N), BF16),
            pltpu.VMEM((steps, 2 * N, N), BF16),
            pltpu.VMEM((steps, TR, N), F32),
            pltpu.VMEM((SEGS, MAP, N), F32),
            pltpu.VMEM((SEGS - 1, MAP, N), F32),
            pltpu.VMEM((ny, MAP, N), F32),
            pltpu.VMEM((max(ny - 1, 1), MAP, N), F32),
            pltpu.VMEM((nc, MAP, N), F32),
            pltpu.VMEM((max(nc - 1, 1), MAP, N), F32),
            pltpu.VMEM((nx, MAP, N), F32),
            pltpu.VMEM((max(nx - 1, 1), MAP, N), F32),
            pltpu.VMEM((nz, ROWS, N), F32),
            pltpu.VMEM((nz, N, N), F32),
            pltpu.VMEM((nz, TR, N), F32),
            pltpu.VMEM((4, each, N), F32),
            pltpu.SemaphoreType.DMA((links,)),
            pltpu.SemaphoreType.DMA((links,)),
        ],
        compiler_params=pltpu.CompilerParams(
            collective_id=1, has_side_effects=True, vmem_limit_bytes=56250000
        ),
        name="smooth",
    )(ids, dyn, smooth, gain, obs)


def body(sizes, observations, dynamics, smoother_gain, gains, regime):
    out = main_call(sizes, regime, dynamics, smoother_gain, gains, observations.reshape(-1, N))
    return out.reshape(observations.shape)


def build(torus):
    sizes = tuple(torus.shape[a] for a in ("track",) + TM)
    placed = (
        P(TM, "track", None),
        P("track", None, None),
        P("track", None, None),
        P("track", None),
        P(TM),
    )
    return jax.shard_map(
        functools.partial(body, sizes),
        mesh=torus,
        in_specs=placed,
        out_specs=P(TM, "track", None),
        check_vma=False,
    )


def solution(mesh):
    return build(Mesh(mesh.devices.reshape(mesh.shape["track"], 8, 4, 2), ("track",) + TM))
```
